512 devices in a mesh: cfg: 16 (over z, core), tm: 32 (over y, x).
Axes of the slice: x: 4, y: 8, z: 8, core: 2. Of those that a mesh axis runs over, the one named last changes fastest.
Arguments:
- linv: bfloat16 [65536, 1024], P(('cfg', 'tm')), parts along dimension 0, as said below
- sub: bfloat16 [65536, 1024], P(('cfg', 'tm')), parts along dimension 0, may hold values from -0.046875 to 0.046875
- owner: int32 [64], P('cfg'), parts along dimension 0, may hold values from 0 to 31, as said below
Outputs:
- diag_cov: bfloat16 [65536, 1024], P(('cfg', 'tm')), parts along dimension 0
- off_cov: bfloat16 [65536, 1024], P(('cfg', 'tm')), parts along dimension 0
- owned_var: float32 [1024, 1024], P(('cfg', 'tm')), parts along dimension 0
The draws below stay inside these ranges and needn't reach their ends.
There are 16 independent parts, one for each index of `cfg`. The reference program is written for one: setup_inputs(seed, part) draws one part's arguments, and reference() takes and returns one part's arrays. A program takes and returns all parts, laid end to end along the dimension named above; each array names one. Nothing has to cross between parts.
Inputs may be any that keep to these rules, and one draw needn't show every extreme that they name: Each block of 1024 rows of linv is lower triangular with a positive diagonal. Exactly two time blocks, adjacent in time, share an owner; all other time blocks have distinct owners, so no owner receives more than 2 blocks and one receives exactly 2.
All inputs are finite; a program needn't handle non-finite values.
Results may differ from the reference program's by a relative error of at most 0.0075.
Values may be sent and summed in bfloat16 or wider, within the bound.
No kernel may reach another device: no remote copies, remote signals or barrier semaphores. Data moves between devices by JAX's collectives and lax.ppermute only.
A program may use at most 64 MiB of HBM per device.

```python
import math
import jax
import jax.numpy as jnp
from jax import lax

B = 1024
TB = 4
SLOTS = 2
N_TM = 32


def lower_factor(factor_key):
    diag_key, low_key = jax.random.split(factor_key, 2)
    diagonal_part = jnp.exp(jax.random.uniform(diag_key, (B,), jnp.float32, math.log(0.6), math.log(1.8)))
    spread = jax.random.normal(low_key, (B, B), jnp.float32)
    lower_part = jnp.tril(spread, -1) * (0.5 / math.sqrt(B))
    return lower_part + jnp.diag(diagonal_part)


def draw_linv(key, part):
    factor_keys = jax.random.split(jax.random.fold_in(key, 11), TB)
    stacked = jax.vmap(lower_factor)(factor_keys)
    return stacked.reshape(TB * B, B).astype(jnp.bfloat16)


def draw_sub(key, part):
    sub_key = jax.random.fold_in(key, 37)
    edge_bound = 1.5 / math.sqrt(B)
    values = jnp.clip(jax.random.normal(sub_key, (TB * B, B), jnp.float32) * (0.8 / math.sqrt(B)), -edge_bound, edge_bound)
    return values.astype(jnp.bfloat16)


def draw_owner(key, part):
    perm_key, pair_key = jax.random.split(jax.random.fold_in(key, 23))
    order_perm = jax.random.permutation(perm_key, N_TM)
    pair_at = jax.random.randint(pair_key, (), 0, TB - 1)
    steps_iota = jnp.arange(TB, dtype=jnp.int32)
    picked = jnp.where(steps_iota <= pair_at, steps_iota, steps_iota - 1)
    return order_perm[picked].astype(jnp.int32)


def setup_inputs(seed: int = 0, part: int = 0) -> dict:
    key_of = jax.random.split(jax.random.key(seed), 4)
    part_keys = jax.random.split(jax.random.fold_in(key_of[3], part), 4)
    linv = draw_linv(jax.random.fold_in(jax.random.fold_in(key_of[3], part), 71), part)
    sub = draw_sub(jax.random.fold_in(jax.random.fold_in(key_of[3], part), 71), part)
    owner = draw_owner(jax.random.fold_in(jax.random.fold_in(key_of[3], part), 71), part)
    return {"linv": linv, "sub": sub, "owner": owner}


def reference(linv, sub, owner):
    contract_first = (((0,), (0,)), ((), ()))
    identity = jnp.eye(B, dtype=jnp.bfloat16)
    carried = identity
    diag_parts = []
    off_parts = []
    for step_index in range(TB - 1, -1, -1):
        factor = linv[step_index * B:(step_index + 1) * B]
        lower_block = sub[step_index * B:(step_index + 1) * B]
        coupling = jnp.dot(lower_block, factor, preferred_element_type=jnp.float32).astype(jnp.bfloat16)
        gram = lax.dot_general(factor, factor, contract_first, preferred_element_type=jnp.float32)
        off_block = (-jnp.dot(carried, coupling, preferred_element_type=jnp.float32)).astype(jnp.bfloat16)
        diag_block = (gram - lax.dot_general(coupling, off_block, contract_first, preferred_element_type=jnp.float32)).astype(jnp.bfloat16)
        diag_parts.insert(0, diag_block)
        off_parts.insert(0, off_block)
        carried = diag_block
    diag_cov = jnp.concatenate(diag_parts, 0)
    off_cov = jnp.concatenate(off_parts, 0)
    variances = jnp.stack([jnp.diagonal(entry_block).astype(jnp.float32) for entry_block in diag_parts])
    positions = jnp.arange(TB, dtype=jnp.int32)
    same_owner = owner[:, None] == owner[None, :]
    earlier = positions[None, :] < positions[:, None]
    slot_rank = jnp.sum(jnp.where(same_owner & earlier, 1, 0).astype(jnp.int32), axis=1).astype(jnp.int32)
    target = (owner * SLOTS + slot_rank).astype(jnp.int32)
    owned_var = jnp.zeros((N_TM * SLOTS, B), jnp.float32).at[target].set(variances)
    return diag_cov, off_cov, owned_var
```

```python
import functools

import jax
import jax.numpy as jnp
from jax import lax
from jax.experimental import pallas as pl
from jax.experimental.pallas import tpu as pltpu
from jax.sharding import PartitionSpec as P

TB = 4
SLOTS = 2
NX = 4
BLK = 128
AXES = ("cfg", "tm")


NN = (((1,), (0,)), ((), ()))
NT = (((1,), (1,)), ((), ()))


def pairs_of(fn, n_cfg, n_tm):
    route = []
    for cfg in range(n_cfg):
        for tm in range(n_tm):
            y, x = divmod(tm, NX)
            to = fn(x, y, cfg % 2)
            if to is not None:
                route.append((cfg * n_tm + tm, cfg * n_tm + to[1] * NX + to[0]))
    return route


def send(value, fn):
    route = pairs_of(fn, lax.axis_size("cfg"), lax.axis_size("tm"))
    return lax.ppermute(value, AXES, route)


def to_replica(x, y, core):
    return (x, y ^ 1) if y % 2 != core else None


def from_replica(x, y, core):
    return (x, y ^ 1) if y % 2 == core else None


def earlier_block(x, y, core):
    return (x, y - 2) if y % 2 == core and y >= 2 else None


def ring(by):
    def fn(x, y, core):
        return ((x - by) % NX, y) if y % 2 == core else None

    return fn


def around(value):
    one = send(value, ring(1))
    three = send(value, ring(3))
    two = send(value, ring(2))
    return [value, one, two, three]


def place():
    x = lax.rem(lax.axis_index("tm"), NX)
    core = lax.rem(lax.axis_index("cfg"), 2)
    return x, core


def cols(block):
    return pl.ds(pl.multiple_of(block * BLK, BLK), BLK)


def rel_block(x, rel):
    q = lax.rem(2 * x + rel, 8)
    return lax.rem(q, 2) * NX + lax.div(q, 2)


def put_send(send_ref, strip, x):
    for h in range(2):
        for step in range(5):
            src = cols(rel_block(x, h + step))
            send_ref[h * BLK:(h + 1) * BLK, step * BLK:(step + 1) * BLK] = strip[
                h * BLK:(h + 1) * BLK, src
            ]


def first_kernel(lo0, lo1, lo2, lo3, p0, p1, p2, p3, l_ref, f_ref, ft_ref, gt_ref, send_ref, strip):
    x, core = place()
    f_ref[...] = jnp.zeros_like(f_ref)
    for r, (own, packed) in enumerate(((lo0, p0), (lo1, p1), (lo2, p2), (lo3, p3))):
        at = lax.rem(x + r, NX)
        l_ref[cols(2 * r + core), :] = own[...]
        l_ref[cols(2 * r + 1 - core), :] = packed[:, 0:1024]
        f_ref[cols(NX + at), :] = packed[:, 1024:2048]
        f_ref[cols(at), 0:512] = packed[:, 2048:2560]
    for h in range(2):
        ft_ref[h * BLK:(h + 1) * BLK, :] = f_ref[:, cols(h * NX + x)].astype(jnp.float32).T.astype(jnp.bfloat16)
    gt_ref[...] = lax.dot_general(
        ft_ref[...], l_ref[...], NT, preferred_element_type=jnp.float32
    ).astype(jnp.bfloat16)
    inner = ft_ref[...].astype(jnp.float32) + lax.dot_general(
        gt_ref[...], l_ref[...], NN, preferred_element_type=jnp.float32
    )
    strip[...] = lax.dot_general(
        inner.astype(jnp.bfloat16), f_ref[...], NN, preferred_element_type=jnp.float32
    ).astype(jnp.bfloat16)
    put_send(send_ref, strip, x)


def second_kernel(l_ref, f_ref, ft_ref, g_ref, d_ref):
    d_ref[...] = lax.dot_general(
        ft_ref[...], f_ref[...], NN, preferred_element_type=jnp.float32
    )

    def body(i, carry):
        rows = pl.ds(pl.multiple_of(i * 256, 256), 256)
        g_ref[rows, :] = lax.dot_general(
            l_ref[rows, :], f_ref[...], NN, preferred_element_type=jnp.float32
        ).astype(jnp.bfloat16)
        return carry

    lax.fori_loop(0, 4, body, 0)


def rebuild(s_ref, pieces, last):
    @pl.when(jnp.logical_not(last))
    def _():
        for r in range(NX):
            for h in range(2):
                a = 2 * r + h
                rows = slice(a * BLK, (a + 1) * BLK)
                for step in range(5):
                    b = (a + step) % 8
                    block = pieces[r][h * BLK:(h + 1) * BLK, step * BLK:(step + 1) * BLK]
                    s_ref[rows, b * BLK:(b + 1) * BLK] = block
                    if 1 <= step <= 3:
                        s_ref[b * BLK:(b + 1) * BLK, rows] = block.astype(jnp.float32).T.astype(jnp.bfloat16)

    @pl.when(last)
    def _():
        def body(i, carry):
            rows = pl.ds(pl.multiple_of(i * BLK, BLK), BLK)
            row = lax.broadcasted_iota(jnp.int32, (BLK, 1024), 0) + i * BLK
            col = lax.broadcasted_iota(jnp.int32, (BLK, 1024), 1)
            s_ref[rows, :] = jnp.where(row == col, 1.0, 0.0).astype(jnp.bfloat16)
            return carry

        lax.fori_loop(0, 8, body, 0)


def new_strip(s_ref, g_ref, gt_ref, d_ref):
    wt = lax.dot_general(gt_ref[...], s_ref[...], NN, preferred_element_type=jnp.float32)
    return d_ref[...] + lax.dot_general(
        wt.astype(jnp.bfloat16), g_ref[...], NN, preferred_element_type=jnp.float32
    )


def is_last():
    return lax.div(lax.axis_index("tm"), 2 * NX) == TB - 1


def step_kernel(p0, p1, p2, p3, g_ref, gt_ref, d_ref, send_ref, s_ref, strip):
    x, _ = place()
    rebuild(s_ref, (p0, p1, p2, p3), is_last())
    strip[...] = new_strip(s_ref, g_ref, gt_ref, d_ref).astype(jnp.bfloat16)
    put_send(send_ref, strip, x)


def final_kernel(p0, p1, p2, p3, g_ref, gt_ref, d_ref, own_ref, par_ref, var_ref, s_ref, strip, off):
    x, core = place()
    rebuild(s_ref, (p0, p1, p2, p3), is_last())
    off[...] = (-lax.dot_general(
        s_ref[0:256, :], g_ref[...], NN, preferred_element_type=jnp.float32
    )).astype(jnp.bfloat16)
    strip[...] = new_strip(s_ref, g_ref, gt_ref, d_ref).astype(jnp.bfloat16)
    own_ref[0] = strip[cols(core), :]
    own_ref[1] = off[cols(core), :]
    par_ref[0] = strip[cols(1 - core), :]
    par_ref[1] = off[cols(1 - core), :]
    row = lax.broadcasted_iota(jnp.int32, (BLK, BLK), 0)
    col = lax.broadcasted_iota(jnp.int32, (BLK, BLK), 1)
    var_ref[...] = jnp.zeros_like(var_ref)
    for h in range(2):
        block = strip[h * BLK:(h + 1) * BLK, cols(h * NX + x)].astype(jnp.float32)
        var_ref[h:h + 1, :] = jnp.sum(jnp.where(row == col, block, 0.0), axis=0, keepdims=True)


def call(kernel, outs, scratch, flops, *args):
    vmem = pl.BlockSpec(memory_space=pltpu.VMEM)
    moved = sum(a.size * a.dtype.itemsize for a in args)
    return pl.pallas_call(
        kernel,
        out_shape=outs,
        in_specs=[vmem] * len(args),
        out_specs=[vmem] * len(outs),
        scratch_shapes=scratch,
        cost_estimate=pl.CostEstimate(flops=flops, bytes_accessed=moved, transcendentals=0),
        compiler_params=pltpu.CompilerParams(vmem_limit_bytes=48 * 1024 * 1024),
    )(*args)


def shards(linv, sub, owner):
    bf16, f32 = jnp.bfloat16, jnp.float32
    shape = jax.ShapeDtypeStruct
    n = linv.shape[1]
    core = lax.rem(lax.axis_index("cfg"), 2)
    tm = lax.axis_index("tm")
    replica = lax.rem(lax.div(tm, NX), 2) == core
    one = 2 * 256 * n * n

    sub_par = send(sub, to_replica)
    linv_par = send(linv, to_replica)
    own_l = around(sub)
    low = jnp.where(core == 0, linv[:, :n // 2], linv_par[:, :n // 2])
    high = jnp.where(core == 0, linv_par, linv)
    packed = around(jnp.concatenate([sub_par, high, low], 1))

    lw, fw, ft, gt, out = call(
        first_kernel,
        [shape((n, n), bf16), shape((n, n), bf16), shape((256, n), bf16), shape((256, n), bf16), shape((256, 640), bf16)],
        [pltpu.VMEM((256, n), bf16)],
        3 * one, *own_l, *packed,
    )
    gw, dm = call(
        second_kernel, [shape((n, n), bf16), shape((256, n), f32)], [], 5 * one, lw, fw, ft
    )
    for turn in range(TB - 1):
        pieces = around(send(out, earlier_block))
        args = (*pieces, gw, gt, dm)
        if turn < TB - 2:
            (out,) = call(
                step_kernel,
                [shape((256, 640), bf16)],
                [pltpu.VMEM((n, n), bf16), pltpu.VMEM((256, n), bf16)],
                2 * one, *args,
            )
        else:
            own, par, var = call(
                final_kernel,
                [shape((2, BLK, n), bf16), shape((2, BLK, n), bf16), shape((8, BLK), f32)],
                [pltpu.VMEM((n, n), bf16), pltpu.VMEM((256, n), bf16), pltpu.VMEM((256, n), bf16)],
                3 * one, *args,
            )
    theirs = send(par, from_replica)
    n_tm = lax.axis_size("tm")
    every = lax.all_to_all(
        jnp.broadcast_to(var[None, 0:2], (n_tm, 2, BLK)), "tm", 0, 0, tiled=True
    ).reshape(TB, 2, NX, 2, BLK)
    kept = jnp.where(core == 0, every[:, 0], every[:, 1])
    variances = kept.transpose(0, 2, 1, 3).reshape(TB, n)
    rows = jnp.where(replica, own, theirs)

    positions = lax.broadcasted_iota(jnp.int32, (TB, TB), 1)
    current = lax.broadcasted_iota(jnp.int32, (TB, TB), 0)
    same_owner = owner[:, None] == owner[None, :]
    rank = jnp.sum(jnp.where(same_owner & (positions < current), 1, 0), axis=1)
    slot = lax.broadcasted_iota(jnp.int32, (SLOTS, TB), 0)
    chosen = (owner[None, :] == tm) & (rank[None, :] == slot)
    owned = jnp.sum(jnp.where(chosen[:, :, None], variances[None], 0.0), axis=1)
    return rows[0], rows[1], owned


def solution(mesh):
    spec = P(AXES, None)
    return jax.shard_map(
        shards,
        mesh=mesh,
        in_specs=(spec, spec, P("cfg")),
        out_specs=(spec, spec, spec),
        check_vma=False,
    )
```

```python
import jax
import jax.numpy as jnp
from jax import lax
from jax.experimental import pallas as pl
from jax.experimental.pallas import tpu as pltpu
from jax.sharding import PartitionSpec as P

TB = 4
SLOTS = 2
NX = 4
N = 1024
BLK = 128
AXES = ("cfg", "tm")
ROW_OF = (0, 3, 5, 6)


NN = (((1,), (0,)), ((), ()))
NT = (((1,), (1,)), ((), ()))
BF16 = jnp.bfloat16
F32 = jnp.float32


def mine(x, core):
    return x // 2 == core


def send(value, fn):
    n_cfg, n_tm = lax.axis_size("cfg"), lax.axis_size("tm")
    route = []
    for cfg in range(n_cfg):
        for tm in range(n_tm):
            y, x = divmod(tm, NX)
            to = fn(x, y, cfg % 2)
            if to is not None:
                route.append((cfg * n_tm + tm, cfg * n_tm + to[1] * NX + to[0]))
    return lax.ppermute(value, AXES, route)


def load_from(dx, parity):
    def fn(x, y, core):
        to = (x - dx) % NX
        return (to, ROW_OF[y // 2]) if y % 2 == parity and mine(to, core) else None

    return fn


def load_above(x, y, core):
    return (x, y ^ 1) if mine(x, core) and y ^ 1 == ROW_OF[y // 2] else None


def replica_to(t, u):
    def fn(x, y, core):
        return (x, ROW_OF[u]) if mine(x, core) and y == ROW_OF[t] else None

    return fn


def spread(across, other):
    def fn(x, y, core):
        if not mine(x, core) or y != ROW_OF[y // 2]:
            return None
        return (3 - x if across else x, y ^ 1 if other else y)

    return fn


def block(b):
    return pl.ds(pl.multiple_of(b * BLK, BLK), BLK)


def tile(i):
    return slice(i * 256, (i + 1) * 256)


def here():
    x = lax.rem(lax.axis_index("tm"), NX)
    y = lax.div(lax.axis_index("tm"), NX)
    return x, lax.rem(y, 2), lax.div(y, 2)


def dot(a, b, dims):
    return lax.dot_general(a, b, dims, preferred_element_type=F32)


def pack(pack_ref, s_ref):
    for p in range(4):
        rows = slice(p * BLK, (p + 1) * BLK)
        width = (8 - p) * BLK
        pack_ref[rows, :width] = s_ref[(7 - p) * BLK:(8 - p) * BLK, :width]
        pack_ref[rows, width:] = s_ref[p * BLK:(p + 1) * BLK, :(p + 1) * BLK]


def unpack(s_ref, pack_ref):
    for p in range(4):
        rows = slice(p * BLK, (p + 1) * BLK)
        width = (8 - p) * BLK
        s_ref[(7 - p) * BLK:(8 - p) * BLK, :width] = pack_ref[rows, :width]
        s_ref[p * BLK:(p + 1) * BLK, :(p + 1) * BLK] = pack_ref[rows, width:]


def mirror(s_ref):
    for i in range(1, 8):
        rows = slice(i * BLK, (i + 1) * BLK)
        left = s_ref[rows, :i * BLK].astype(F32)
        s_ref[:i * BLK, rows] = left.T.astype(BF16)


def pack_upper(pack_ref, f_ref):
    for p in range(4):
        rows = slice(p * BLK, (p + 1) * BLK)
        width = (8 - p) * BLK
        pack_ref[rows, :width] = f_ref[p * BLK:(p + 1) * BLK, p * BLK:]
        pack_ref[rows, width:] = f_ref[(7 - p) * BLK:(8 - p) * BLK, (7 - p) * BLK:]


def unpack_upper(f_ref, pack_ref):
    f_ref[...] = jnp.zeros_like(f_ref)
    for p in range(4):
        rows = slice(p * BLK, (p + 1) * BLK)
        width = (8 - p) * BLK
        f_ref[p * BLK:(p + 1) * BLK, p * BLK:] = pack_ref[rows, :width]
        f_ref[(7 - p) * BLK:(8 - p) * BLK, (7 - p) * BLK:] = pack_ref[rows, width:]


def lower(s_ref, f_ref, wt_ref, gt_ref):
    for i in range(4):
        cols = slice(0, (i + 1) * 256)
        gram = dot(f_ref[tile(i), i * 256:], f_ref[cols, i * 256:], NT)
        s_ref[tile(i), cols] = (gram + dot(wt_ref[tile(i), :], gt_ref[cols, :], NT)).astype(BF16)


def load_kernel(own_l, own_f, q0, e1, e2, e3, o1, o2, o3, gt_ref, f_ref, fpack_ref, spack_ref, l_ref, s_ref):
    x, parity, _ = here()
    f_ref[512:, :512] = jnp.zeros((512, 512), BF16)

    def place(at, piece, blocks):
        l_ref[block(at), :] = piece[:, :N]
        for b in range(blocks):
            f_ref[b * BLK:(b + 1) * BLK, block(at)] = piece[:, N + b * BLK:N + (b + 1) * BLK]

    at = parity * NX + x
    l_ref[block(at), :] = own_l[...]
    for b in range(8):
        f_ref[b * BLK:(b + 1) * BLK, block(at)] = own_f[:, b * BLK:(b + 1) * BLK]
    place((1 - parity) * NX + x, q0, 8)
    for dx, even, odd in ((1, e1, o1), (2, e2, o2), (3, e3, o3)):
        place(lax.rem(x + dx, NX), even, 4)
        place(NX + lax.rem(x + dx, NX), odd, 8)
    for i in range(4):
        gt_ref[tile(i), :] = dot(f_ref[tile(i), i * 256:], l_ref[:, i * 256:], NT).astype(BF16)
    lower(s_ref, f_ref, gt_ref, gt_ref)
    pack(spack_ref, s_ref)
    pack_upper(fpack_ref, f_ref)


def step_kernel(pack_in, gt_ref, f_ref, pack_out, s_ref, wt_ref):
    unpack(s_ref, pack_in)
    mirror(s_ref)
    for i in range(4):
        wt_ref[tile(i), :] = dot(gt_ref[tile(i), :], s_ref[...], NN).astype(BF16)
    lower(s_ref, f_ref, wt_ref, gt_ref)
    pack(pack_out, s_ref)


def final_kernel(
    to2, to1, to0, gt_next, fpack_next, gt_ref, f_ref, own_ref, a1_ref, a2_ref, a3_ref, var_ref,
    s_ref, wt_ref, fn_ref, gm_ref, fm_ref, sm_ref,
):
    x, parity, group = here()
    for t, source in ((2, to2), (1, to1), (0, to0)):
        @pl.when(group == t)
        def _():
            unpack(s_ref, source)
            mirror(s_ref)

    @pl.when(group == TB - 1)
    def _():
        for i in range(8):
            row = lax.broadcasted_iota(jnp.int32, (BLK, N), 0) + i * BLK
            col = lax.broadcasted_iota(jnp.int32, (BLK, N), 1)
            s_ref[i * BLK:(i + 1) * BLK, :] = jnp.where(row == col, 1.0, 0.0).astype(BF16)

    @pl.when(group == 0)
    def _():
        unpack_upper(fn_ref, fpack_next)
        for i in range(4):
            wt_ref[tile(i), :] = dot(gt_next[tile(i), :], s_ref[...], NN).astype(BF16)
        lower(s_ref, fn_ref, wt_ref, gt_next)
        mirror(s_ref)

    far = 3 - x
    places = (
        parity * NX + x, (1 - parity) * NX + x, parity * NX + far, (1 - parity) * NX + far
    )
    outs = (own_ref, a1_ref, a2_ref, a3_ref)
    for k, at in enumerate(places):
        rows = slice(k * BLK, (k + 1) * BLK)
        gm_ref[rows, :] = gt_ref[block(at), :]
        fm_ref[rows, :] = f_ref[block(at), :]
        sm_ref[rows, :] = s_ref[block(at), :]
    for i in range(2):
        off = -dot(sm_ref[tile(i), :], gt_ref[...], NT)
        outs[2 * i][1] = off[:BLK].astype(BF16)
        outs[2 * i + 1][1] = off[BLK:].astype(BF16)
    for i in range(2):
        wt = dot(gm_ref[tile(i), :], s_ref[...], NN).astype(BF16)
        strip = dot(fm_ref[tile(i), :], f_ref[...], NT) + dot(wt, gt_ref[...], NT)
        outs[2 * i][0] = strip[:BLK].astype(BF16)
        outs[2 * i + 1][0] = strip[BLK:].astype(BF16)
    row = lax.broadcasted_iota(jnp.int32, (BLK, BLK), 0)
    col = lax.broadcasted_iota(jnp.int32, (BLK, BLK), 1)
    var_ref[...] = jnp.zeros_like(var_ref)
    for k, at in enumerate(places):
        square = outs[k][0, :, block(at)].astype(F32)
        var_ref[pl.ds(at, 1), :] = jnp.sum(jnp.where(row == col, square, 0.0), axis=0, keepdims=True)


def call(kernel, outs, scratch, flops, *args):
    vmem = pl.BlockSpec(memory_space=pltpu.VMEM)
    moved = sum(a.size * a.dtype.itemsize for a in args)
    return pl.pallas_call(
        kernel,
        out_shape=[jax.ShapeDtypeStruct(s, d) for s, d in outs],
        in_specs=[vmem] * len(args),
        out_specs=[vmem] * len(outs),
        scratch_shapes=[pltpu.VMEM(s, BF16) for s in scratch],
        cost_estimate=pl.CostEstimate(flops=flops, bytes_accessed=moved, transcendentals=0),
        compiler_params=pltpu.CompilerParams(vmem_limit_bytes=24 * 1024 * 1024),
    )(*args)


def shards(linv, sub, owner):
    core = lax.rem(lax.axis_index("cfg"), 2)
    tm = lax.axis_index("tm")
    x, y = lax.rem(tm, NX), lax.div(tm, NX)
    flops = 2 * N * N * N
    square, packed = (N, N), (512, 1152)

    turned = linv.reshape(BLK, 8, BLK).transpose(2, 1, 0).reshape(BLK, N)
    full = jnp.concatenate([sub, turned], 1)
    short = full[:, :N + 512]
    q0 = send(full, load_above)
    evens = [send(short, load_from(dx, 0)) for dx in (1, 2, 3)]
    odds = [send(full, load_from(dx, 1)) for dx in (1, 2, 3)]
    gt, ft, fpack, spack = call(
        load_kernel,
        [(square, BF16), (square, BF16), (packed, BF16), (packed, BF16)],
        [square, square], 3 * flops, sub, turned, q0, *evens, *odds,
    )
    to2 = send(spack, replica_to(3, 2))
    gt_next = send(gt, replica_to(1, 0))
    f_next = send(fpack, replica_to(1, 0))
    (second,) = call(step_kernel, [(packed, BF16)], [square, square], 2 * flops, to2, gt, ft)
    to1 = send(second, replica_to(2, 1))
    to0 = send(second, replica_to(2, 0))
    strip = (2, BLK, N)
    own, a1, a2, a3, var = call(
        final_kernel,
        [(strip, BF16)] * 4 + [((8, BLK), F32)],
        [square, square, square, (512, N), (512, N), (512, N)],
        4 * flops, to2, to1, to0, gt_next, f_next, gt, ft,
    )
    b1 = send(a1, spread(False, True))
    b2 = send(a2, spread(True, False))
    b3 = send(a3, spread(True, True))

    n_tm = lax.axis_size("tm")
    every = lax.all_to_all(
        jnp.broadcast_to(var[None], (n_tm, 8, BLK)), "tm", 0, 0, tiled=True
    ).reshape(2 * TB, NX, 8, BLK)
    both = jnp.stack([every[r] for r in ROW_OF])
    pair = jnp.where(core == 0, both[:, 0] + both[:, 1], both[:, 2] + both[:, 3])
    variances = pair.reshape(TB, N)

    near = lax.div(x, 2) == core
    row_of = sum(jnp.where(lax.div(y, 2) == t, ROW_OF[t], 0) for t in range(TB))
    level = y == row_of
    rows = jnp.where(near, jnp.where(level, own, b1), jnp.where(level, b2, b3))

    positions = lax.broadcasted_iota(jnp.int32, (TB, TB), 1)
    current = lax.broadcasted_iota(jnp.int32, (TB, TB), 0)
    same_owner = owner[:, None] == owner[None, :]
    rank = jnp.sum(jnp.where(same_owner & (positions < current), 1, 0), axis=1)
    slot = lax.broadcasted_iota(jnp.int32, (SLOTS, TB), 0)
    chosen = (owner[None, :] == tm) & (rank[None, :] == slot)
    owned = jnp.sum(jnp.where(chosen[:, :, None], variances[None], 0.0), axis=1)
    return rows[0], rows[1], owned


def solution(mesh):
    spec = P(AXES, None)
    return jax.shard_map(
        shards,
        mesh=mesh,
        in_specs=(spec, spec, P("cfg")),
        out_specs=(spec, spec, spec),
        check_vma=False,
    )
```

```python
import jax
import jax.numpy as jnp
from jax import lax
from jax.experimental import pallas as pl
from jax.experimental.pallas import tpu as pltpu
from jax.sharding import PartitionSpec as P


TB = 4
SLOTS = 2
NX = 4
N = 1024
BLK = 128
AXES = ("cfg", "tm")
ROW_OF = ((0, 3, 5, 6), (0, 2, 5, 7))


NN = (((1,), (0,)), ((), ()))
NT = (((1,), (1,)), ((), ()))
BF16 = jnp.bfloat16
F32 = jnp.float32


def mine(x, core):
    return x // 2 == core


def send(value, fn):
    n_cfg, n_tm = lax.axis_size("cfg"), lax.axis_size("tm")
    route = []
    for cfg in range(n_cfg):
        for tm in range(n_tm):
            y, x = divmod(tm, NX)
            to = fn(x, y, cfg % 2)
            if to is not None:
                route.append((cfg * n_tm + tm, cfg * n_tm + to[1] * NX + to[0]))
    return lax.ppermute(value, AXES, route)


def load_from(dx, parity):
    def fn(x, y, core):
        to = (x - dx) % NX
        return (to, ROW_OF[core][y // 2]) if y % 2 == parity and mine(to, core) else None

    return fn


def load_above(x, y, core):
    return (x, y ^ 1) if mine(x, core) and y ^ 1 == ROW_OF[core][y // 2] else None


def replica_to(t, u):
    def fn(x, y, core):
        return (x, ROW_OF[core][u]) if mine(x, core) and y == ROW_OF[core][t] else None

    return fn


def spread(across, other):
    def fn(x, y, core):
        if not mine(x, core) or y != ROW_OF[core][y // 2]:
            return None
        return (3 - x if across else x, y ^ 1 if other else y)

    return fn


def block(b):
    return pl.ds(pl.multiple_of(b * BLK, BLK), BLK)


def tile(i):
    return slice(i * 256, (i + 1) * 256)


def here():
    x = lax.rem(lax.axis_index("tm"), NX)
    y = lax.div(lax.axis_index("tm"), NX)
    return x, lax.rem(y, 2), lax.div(y, 2)


def dot(a, b, dims):
    return lax.dot_general(a, b, dims, preferred_element_type=F32)


def pack(pack_ref, s_ref):
    for p in range(4):
        rows = slice(p * BLK, (p + 1) * BLK)
        width = (8 - p) * BLK
        pack_ref[rows, :width] = s_ref[(7 - p) * BLK:(8 - p) * BLK, :width]
        pack_ref[rows, width:] = s_ref[p * BLK:(p + 1) * BLK, :(p + 1) * BLK]


def unpack(s_ref, pack_ref):
    for p in range(4):
        rows = slice(p * BLK, (p + 1) * BLK)
        width = (8 - p) * BLK
        s_ref[(7 - p) * BLK:(8 - p) * BLK, :width] = pack_ref[rows, :width]
        s_ref[p * BLK:(p + 1) * BLK, :(p + 1) * BLK] = pack_ref[rows, width:]


def mirror(s_ref):
    for i in range(1, 8):
        rows = slice(i * BLK, (i + 1) * BLK)
        left = s_ref[rows, :i * BLK].astype(F32)
        s_ref[:i * BLK, rows] = left.T.astype(BF16)


def pack_upper(pack_ref, f_ref):
    for p in range(4):
        rows = slice(p * BLK, (p + 1) * BLK)
        width = (8 - p) * BLK
        pack_ref[rows, :width] = f_ref[p * BLK:(p + 1) * BLK, p * BLK:]
        pack_ref[rows, width:] = f_ref[(7 - p) * BLK:(8 - p) * BLK, (7 - p) * BLK:]


def unpack_upper(f_ref, pack_ref):
    f_ref[...] = jnp.zeros_like(f_ref)
    for p in range(4):
        rows = slice(p * BLK, (p + 1) * BLK)
        width = (8 - p) * BLK
        f_ref[p * BLK:(p + 1) * BLK, p * BLK:] = pack_ref[rows, :width]
        f_ref[(7 - p) * BLK:(8 - p) * BLK, (7 - p) * BLK:] = pack_ref[rows, width:]


def lower(s_ref, f_ref, wt_ref, gt_ref):
    for i in range(4):
        cols = slice(0, (i + 1) * 256)
        gram = dot(f_ref[tile(i), i * 256:], f_ref[cols, i * 256:], NT)
        s_ref[tile(i), cols] = (gram + dot(wt_ref[tile(i), :], gt_ref[cols, :], NT)).astype(BF16)


def load_kernel(own_l, own_f, q0, e1, e2, e3, o1, o2, o3, gt_ref, f_ref, fpack_ref, spack_ref, l_ref, s_ref):
    x, parity, _ = here()
    f_ref[512:, :512] = jnp.zeros((512, 512), BF16)

    def place(at, piece, blocks):
        l_ref[block(at), :] = piece[:, :N]
        for b in range(blocks):
            f_ref[b * BLK:(b + 1) * BLK, block(at)] = piece[:, N + b * BLK:N + (b + 1) * BLK]

    at = parity * NX + x
    l_ref[block(at), :] = own_l[...]
    for b in range(8):
        f_ref[b * BLK:(b + 1) * BLK, block(at)] = own_f[:, b * BLK:(b + 1) * BLK]
    place((1 - parity) * NX + x, q0, 8)
    for dx, even, odd in ((1, e1, o1), (2, e2, o2), (3, e3, o3)):
        place(lax.rem(x + dx, NX), even, 4)
        place(NX + lax.rem(x + dx, NX), odd, 8)
    for i in range(4):
        gt_ref[tile(i), :] = dot(f_ref[tile(i), i * 256:], l_ref[:, i * 256:], NT).astype(BF16)
    lower(s_ref, f_ref, gt_ref, gt_ref)
    pack(spack_ref, s_ref)
    pack_upper(fpack_ref, f_ref)


def step_kernel(pack_in, gt_ref, f_ref, pack_out, s_ref, wt_ref):
    unpack(s_ref, pack_in)
    mirror(s_ref)
    for i in range(4):
        wt_ref[tile(i), :] = dot(gt_ref[tile(i), :], s_ref[...], NN).astype(BF16)
    lower(s_ref, f_ref, wt_ref, gt_ref)
    pack(pack_out, s_ref)


def rows_of(x, parity):
    far = 3 - x
    return (
        parity * NX + x, (1 - parity) * NX + x, parity * NX + far, (1 - parity) * NX + far
    )


def pick(out_ref, at, ref, places):
    for k, place in enumerate(places):
        out_ref[at + k * BLK:at + (k + 1) * BLK, :] = ref[block(place), :]


def gram_kernel(f_ref, out_ref, fm_ref):
    x, parity, _ = here()
    pick(fm_ref, 0, f_ref, rows_of(x, parity))
    for i in range(2):
        out_ref[tile(i), :] = dot(fm_ref[tile(i), :], f_ref[...], NT)


def prepare_kernel(gt_next, fpack_next, gt_ref, left_ref, base_ref, fn_ref, gm_ref, h_ref):
    x, parity, _ = here()
    places = rows_of(x, parity)
    unpack_upper(fn_ref, fpack_next)
    pick(gm_ref, 0, gt_ref, places)
    pick(left_ref, 512, gt_next, places)
    pick(h_ref, 512, fn_ref, places)
    for i in range(2):
        left_ref[tile(i), :] = dot(gm_ref[tile(i), :], gt_next[...], NN).astype(BF16)
        h_ref[tile(i), :] = dot(gm_ref[tile(i), :], fn_ref[...], NN).astype(BF16)
    for i in range(4):
        base_ref[tile(i), :] = dot(h_ref[tile(i), :], fn_ref[...], NT)


def final_kernel(
    to2, to1, to0, left_ref, base_ref, gt_next, gram_ref, gt_ref,
    own_ref, a1_ref, a2_ref, a3_ref, var_ref, s_ref, x_ref, w_ref,
):
    x, parity, group = here()
    places = rows_of(x, parity)
    for t, source in ((2, to2), (1, to1), (0, to0)):
        @pl.when(group == t)
        def _():
            unpack(s_ref, source)
            mirror(s_ref)

    @pl.when(group == TB - 1)
    def _():
        for i in range(8):
            row = lax.broadcasted_iota(jnp.int32, (BLK, N), 0) + i * BLK
            col = lax.broadcasted_iota(jnp.int32, (BLK, N), 1)
            s_ref[i * BLK:(i + 1) * BLK, :] = jnp.where(row == col, 1.0, 0.0).astype(BF16)

    @pl.when(group == 0)
    def _():
        for i in range(4):
            w_ref[tile(i), :] = dot(left_ref[tile(i), :], s_ref[...], NN).astype(BF16)
        for i in range(4):
            x_ref[tile(i), :] = (base_ref[tile(i), :] + dot(w_ref[tile(i), :], gt_next[...], NT)).astype(BF16)

    @pl.when(group != 0)
    def _():
        pick(w_ref, 0, gt_ref, places)
        for i in range(2):
            x_ref[tile(i), :] = dot(w_ref[tile(i), :], s_ref[...], NN).astype(BF16)
        pick(x_ref, 512, s_ref, places)

    outs = (own_ref, a1_ref, a2_ref, a3_ref)
    for i in range(2):
        strip = gram_ref[tile(i), :] + dot(x_ref[tile(i), :], gt_ref[...], NT)
        outs[2 * i][0] = strip[:BLK].astype(BF16)
        outs[2 * i + 1][0] = strip[BLK:].astype(BF16)
        off = -dot(x_ref[tile(i + 2), :], gt_ref[...], NT)
        outs[2 * i][1] = off[:BLK].astype(BF16)
        outs[2 * i + 1][1] = off[BLK:].astype(BF16)
    row = lax.broadcasted_iota(jnp.int32, (BLK, BLK), 0)
    col = lax.broadcasted_iota(jnp.int32, (BLK, BLK), 1)
    var_ref[...] = jnp.zeros_like(var_ref)
    for k, at in enumerate(places):
        square = outs[k][0, :, block(at)].astype(F32)
        var_ref[pl.ds(at, 1), :] = jnp.sum(jnp.where(row == col, square, 0.0), axis=0, keepdims=True)


def call(kernel, outs, scratch, flops, *args):
    vmem = pl.BlockSpec(memory_space=pltpu.VMEM)
    moved = sum(a.size * a.dtype.itemsize for a in args)
    return pl.pallas_call(
        kernel,
        out_shape=[jax.ShapeDtypeStruct(s, d) for s, d in outs],
        in_specs=[vmem] * len(args),
        out_specs=[vmem] * len(outs),
        scratch_shapes=[pltpu.VMEM(s, BF16) for s in scratch],
        cost_estimate=pl.CostEstimate(flops=flops, bytes_accessed=moved, transcendentals=0),
        compiler_params=pltpu.CompilerParams(vmem_limit_bytes=24 * 1024 * 1024),
    )(*args)


def sweep(linv, sub, owner):
    core = lax.rem(lax.axis_index("cfg"), 2)
    tm = lax.axis_index("tm")
    x, y = lax.rem(tm, NX), lax.div(tm, NX)
    flops = 2 * N * N * N
    square, packed, half = (N, N), (512, 1152), (512, N)

    turned = linv.reshape(BLK, 8, BLK).transpose(2, 1, 0).reshape(BLK, N)
    full = jnp.concatenate([sub, turned], 1)
    short = full[:, :N + 512]
    q0 = send(full, load_above)
    evens = [send(short, load_from(dx, 0)) for dx in (1, 2, 3)]
    odds = [send(full, load_from(dx, 1)) for dx in (1, 2, 3)]
    gt, ft, fpack, spack = call(
        load_kernel,
        [(square, BF16), (square, BF16), (packed, BF16), (packed, BF16)],
        [square, square], 3 * flops, sub, turned, q0, *evens, *odds,
    )
    to2 = send(spack, replica_to(3, 2))
    gt_next = send(gt, replica_to(1, 0))
    f_next = send(fpack, replica_to(1, 0))
    (second,) = call(step_kernel, [(packed, BF16)], [square, square], 2 * flops, to2, gt, ft)
    to0 = send(second, replica_to(2, 0))
    to1 = send(second, replica_to(2, 1))
    (gram,) = call(gram_kernel, [(half, F32)], [half], flops, ft)
    left, base = call(
        prepare_kernel, [(square, BF16), (square, F32)], [square, half, square],
        2 * flops, gt_next, f_next, gt,
    )
    strip = (2, BLK, N)
    own, a1, a2, a3, var = call(
        final_kernel,
        [(strip, BF16)] * 4 + [((8, BLK), F32)],
        [square, square, square],
        4 * flops, to2, to1, to0, left, base, gt_next, gram, gt,
    )
    b1 = send(a1, spread(False, True))
    b3 = send(a3, spread(True, True))
    b2 = send(a2, spread(True, False))

    n_tm = lax.axis_size("tm")
    every = lax.all_to_all(
        jnp.broadcast_to(var[None], (n_tm, 8, BLK)), "tm", 0, 0, tiled=True
    )
    every = every.reshape(2 * TB, NX, 8, BLK)
    pair = jnp.stack([
        jnp.where(core == 0, every[r0, 0] + every[r0, 1], every[r1, 2] + every[r1, 3])
        for r0, r1 in zip(*ROW_OF)
    ])
    variances = pair.reshape(TB, N)

    near = lax.div(x, 2) == core
    row_of = sum(
        jnp.where(lax.div(y, 2) == t, jnp.where(core == 0, ROW_OF[0][t], ROW_OF[1][t]), 0)
        for t in range(TB)
    )
    level = y == row_of
    rows = [
        jnp.where(near, jnp.where(level, own[i], b1[i]), jnp.where(level, b2[i], b3[i]))
        for i in range(2)
    ]

    positions = lax.broadcasted_iota(jnp.int32, (TB, TB), 1)
    current = lax.broadcasted_iota(jnp.int32, (TB, TB), 0)
    same_owner = owner[:, None] == owner[None, :]
    rank = jnp.sum(jnp.where(same_owner & (positions < current), 1, 0), axis=1)
    slot = lax.broadcasted_iota(jnp.int32, (SLOTS, TB), 0)
    chosen = (owner[None, :] == tm) & (rank[None, :] == slot)
    owned = jnp.sum(jnp.where(chosen[:, :, None], variances[None], 0.0), axis=1)
    return rows[0], rows[1], owned


def solution(mesh):
    spec = P(AXES, None)
    return jax.shard_map(
        sweep,
        mesh=mesh,
        in_specs=(spec, spec, P("cfg")),
        out_specs=(spec, spec, spec),
        check_vma=False,
    )
```

```python
import jax
import jax.numpy as jnp
from jax import lax
from jax.experimental import pallas as pl
from jax.experimental.pallas import tpu as pltpu
from jax.sharding import PartitionSpec as P


TB = 4
SLOTS = 2
NX = 4
N = 1024
BLK = 128
AXES = ("cfg", "tm")
ROW_OF = ((0, 3, 5, 6), (0, 2, 5, 7))


NN = (((1,), (0,)), ((), ()))
NT = (((1,), (1,)), ((), ()))
BF16 = jnp.bfloat16
F32 = jnp.float32


def mine(x, core):
    return x // 2 == core


def send(value, fn):
    n_cfg, n_tm = lax.axis_size("cfg"), lax.axis_size("tm")
    route = []
    for cfg in range(n_cfg):
        for tm in range(n_tm):
            y, x = divmod(tm, NX)
            to = fn(x, y, cfg % 2)
            if to is not None:
                route.append((cfg * n_tm + tm, cfg * n_tm + to[1] * NX + to[0]))
    return lax.ppermute(value, AXES, route)


def load_from(dx, parity):
    def fn(x, y, core):
        to = (x - dx) % NX
        return (to, ROW_OF[core][y // 2]) if y % 2 == parity and mine(to, core) else None

    return fn


def load_above(x, y, core):
    return (x, y ^ 1) if mine(x, core) and y ^ 1 == ROW_OF[core][y // 2] else None


def replica_to(t, u):
    def fn(x, y, core):
        return (x, ROW_OF[core][u]) if mine(x, core) and y == ROW_OF[core][t] else None

    return fn


def spread(across, other):
    def fn(x, y, core):
        if not mine(x, core) or y != ROW_OF[core][y // 2]:
            return None
        return (3 - x if across else x, y ^ 1 if other else y)

    return fn


def block(b):
    return pl.ds(pl.multiple_of(b * BLK, BLK), BLK)


def tile(i):
    return slice(i * 256, (i + 1) * 256)


def here():
    x = lax.rem(lax.axis_index("tm"), NX)
    y = lax.div(lax.axis_index("tm"), NX)
    return x, lax.rem(y, 2), lax.div(y, 2)


def dot(a, b, dims):
    return lax.dot_general(a, b, dims, preferred_element_type=F32)


def pack(pack_ref, s_ref):
    for p in range(4):
        rows = slice(p * BLK, (p + 1) * BLK)
        width = (8 - p) * BLK
        pack_ref[rows, :width] = s_ref[(7 - p) * BLK:(8 - p) * BLK, :width]
        pack_ref[rows, width:] = s_ref[p * BLK:(p + 1) * BLK, :(p + 1) * BLK]


def unpack(s_ref, pack_ref):
    for p in range(4):
        rows = slice(p * BLK, (p + 1) * BLK)
        width = (8 - p) * BLK
        s_ref[(7 - p) * BLK:(8 - p) * BLK, :width] = pack_ref[rows, :width]
        s_ref[p * BLK:(p + 1) * BLK, :(p + 1) * BLK] = pack_ref[rows, width:]


def mirror(s_ref):
    for i in range(1, 8):
        rows = slice(i * BLK, (i + 1) * BLK)
        left = s_ref[rows, :i * BLK].astype(F32)
        s_ref[:i * BLK, rows] = left.T.astype(BF16)


def pack_upper(pack_ref, f_ref):
    for p in range(4):
        rows = slice(p * BLK, (p + 1) * BLK)
        width = (8 - p) * BLK
        pack_ref[rows, :width] = f_ref[p * BLK:(p + 1) * BLK, p * BLK:]
        pack_ref[rows, width:] = f_ref[(7 - p) * BLK:(8 - p) * BLK, (7 - p) * BLK:]


def unpack_upper(f_ref, pack_ref):
    f_ref[...] = jnp.zeros_like(f_ref)
    for p in range(4):
        rows = slice(p * BLK, (p + 1) * BLK)
        width = (8 - p) * BLK
        f_ref[p * BLK:(p + 1) * BLK, p * BLK:] = pack_ref[rows, :width]
        f_ref[(7 - p) * BLK:(8 - p) * BLK, (7 - p) * BLK:] = pack_ref[rows, width:]


def lower(s_ref, f_ref, wt_ref, gt_ref):
    for i in range(4):
        cols = slice(0, (i + 1) * 256)
        gram = dot(f_ref[tile(i), i * 256:], f_ref[cols, i * 256:], NT)
        s_ref[tile(i), cols] = (gram + dot(wt_ref[tile(i), :], gt_ref[cols, :], NT)).astype(BF16)


def pack_kernel(linv_ref, sub_ref, full_ref, short_ref):
    full_ref[:, :N] = sub_ref[...]
    short_ref[:, :N] = sub_ref[...]
    for b in range(8):
        turned = linv_ref[:, b * BLK:(b + 1) * BLK].astype(F32).T.astype(BF16)
        full_ref[:, N + b * BLK:N + (b + 1) * BLK] = turned
        if b < 4:
            short_ref[:, N + b * BLK:N + (b + 1) * BLK] = turned


def load_kernel(own, q0, e1, e2, e3, o1, o2, o3, gt_ref, f_ref, fpack_ref, spack_ref, l_ref, s_ref):
    x, parity, _ = here()
    f_ref[512:, :512] = jnp.zeros((512, 512), BF16)

    def place(at, piece, blocks):
        l_ref[block(at), :] = piece[:, :N]
        for b in range(blocks):
            f_ref[b * BLK:(b + 1) * BLK, block(at)] = piece[:, N + b * BLK:N + (b + 1) * BLK]

    place(parity * NX + x, own, 8)
    place((1 - parity) * NX + x, q0, 8)
    for dx, even, odd in ((1, e1, o1), (2, e2, o2), (3, e3, o3)):
        place(lax.rem(x + dx, NX), even, 4)
        place(NX + lax.rem(x + dx, NX), odd, 8)
    for i in range(4):
        gt_ref[tile(i), :] = dot(f_ref[tile(i), i * 256:], l_ref[:, i * 256:], NT).astype(BF16)
    lower(s_ref, f_ref, gt_ref, gt_ref)
    pack(spack_ref, s_ref)
    pack_upper(fpack_ref, f_ref)


def step_kernel(pack_in, gt_ref, f_ref, pack_out, s_ref, wt_ref):
    unpack(s_ref, pack_in)
    mirror(s_ref)
    for i in range(4):
        wt_ref[tile(i), :] = dot(gt_ref[tile(i), :], s_ref[...], NN).astype(BF16)
    lower(s_ref, f_ref, wt_ref, gt_ref)
    pack(pack_out, s_ref)


def rows_of(x, parity):
    far = 3 - x
    return (
        parity * NX + x, (1 - parity) * NX + x, parity * NX + far, (1 - parity) * NX + far
    )


def pick(out_ref, at, ref, places):
    for k, place in enumerate(places):
        out_ref[at + k * BLK:at + (k + 1) * BLK, :] = ref[block(place), :]


def gram_kernel(f_ref, out_ref, fm_ref):
    x, parity, _ = here()
    pick(fm_ref, 0, f_ref, rows_of(x, parity))
    for i in range(2):
        out_ref[tile(i), :] = dot(fm_ref[tile(i), :], f_ref[...], NT)


def base_kernel(fpack_next, gt_ref, base_ref, fn_ref, gm_ref, h_ref):
    x, parity, _ = here()
    places = rows_of(x, parity)
    unpack_upper(fn_ref, fpack_next)
    pick(gm_ref, 0, gt_ref, places)
    pick(h_ref, 512, fn_ref, places)
    for i in range(2):
        h_ref[tile(i), :] = dot(gm_ref[tile(i), :], fn_ref[...], NN).astype(BF16)
    for i in range(4):
        base_ref[tile(i), :] = dot(h_ref[tile(i), :], fn_ref[...], NT)


def left_kernel(gt_next, gt_ref, left_ref, gm_ref):
    x, parity, _ = here()
    places = rows_of(x, parity)
    pick(gm_ref, 0, gt_ref, places)
    pick(left_ref, 512, gt_next, places)
    for i in range(2):
        left_ref[tile(i), :] = dot(gm_ref[tile(i), :], gt_next[...], NN).astype(BF16)


def sweep_kernel(
    to2, to1, to0, left_ref, base_ref, gt_next, gram_ref, gt_ref,
    own_ref, a1_ref, a2_ref, a3_ref, var_ref, s_ref, w_ref, x_ref, d_ref,
):
    x, parity, group = here()
    places = rows_of(x, parity)
    for t, source in ((2, to2), (1, to1), (0, to0)):
        @pl.when(group == t)
        def _():
            unpack(s_ref, source)
            mirror(s_ref)

    @pl.when(group == TB - 1)
    def _():
        for i in range(8):
            row = lax.broadcasted_iota(jnp.int32, (BLK, N), 0) + i * BLK
            col = lax.broadcasted_iota(jnp.int32, (BLK, N), 1)
            s_ref[i * BLK:(i + 1) * BLK, :] = jnp.where(row == col, 1.0, 0.0).astype(BF16)

    @pl.when(group == 0)
    def _():
        for i in range(4):
            w_ref[tile(i), :] = dot(left_ref[tile(i), :], s_ref[...], NN).astype(BF16)
        for i in range(4):
            x_ref[tile(i), :] = (base_ref[tile(i), :] + dot(w_ref[tile(i), :], gt_next[...], NT)).astype(BF16)

    @pl.when(group != 0)
    def _():
        pick(w_ref, 0, gt_ref, places)
        for i in range(2):
            x_ref[tile(i), :] = dot(w_ref[tile(i), :], s_ref[...], NN).astype(BF16)
        pick(x_ref, 512, s_ref, places)

    row = lax.broadcasted_iota(jnp.int32, (BLK, BLK), 0)
    col = lax.broadcasted_iota(jnp.int32, (BLK, BLK), 1)
    d_ref[...] = jnp.zeros_like(d_ref)
    for k, at in enumerate(places):
        rows = slice(k * BLK, (k + 1) * BLK)
        terms = x_ref[rows, :].astype(F32) * gt_ref[block(at), :].astype(F32)
        total = jnp.sum(terms, axis=1, keepdims=True) + gram_ref[rows, block(at)]
        diag = jnp.sum(jnp.where(row == col, total, 0.0), axis=0, keepdims=True)
        d_ref[pl.ds(at, 1), :] = diag.astype(BF16).astype(F32)
    for k in range(var_ref.shape[0]):
        var_ref[k] = d_ref[...]

    outs = (own_ref, a1_ref, a2_ref, a3_ref)
    for i in range(2):
        strip = gram_ref[tile(i), :] + dot(x_ref[tile(i), :], gt_ref[...], NT)
        outs[2 * i][0] = strip[:BLK].astype(BF16)
        outs[2 * i + 1][0] = strip[BLK:].astype(BF16)
        off = -dot(x_ref[tile(i + 2), :], gt_ref[...], NT)
        outs[2 * i][1] = off[:BLK].astype(BF16)
        outs[2 * i + 1][1] = off[BLK:].astype(BF16)


def deliver_kernel(owner_ref, every_ref, own_ref, b1_ref, b2_ref, b3_ref, diag_ref, off_ref, owned_ref):
    x, parity, group = here()
    core = lax.rem(lax.axis_index("cfg"), 2)
    tm = lax.axis_index("tm")

    def by_core(rows):
        return jnp.where(core == 0, rows[0], rows[1])

    level = jnp.int32(0)
    for t in range(TB):
        level = jnp.where(group == t, by_core((ROW_OF[0][t] % 2, ROW_OF[1][t] % 2)), level)
    across = (lax.div(x, 2) != core).astype(jnp.int32)
    way = 2 * across + (parity != level).astype(jnp.int32)
    for k, source in enumerate((own_ref, b1_ref, b2_ref, b3_ref)):
        @pl.when(way == k)
        def _():
            diag_ref[...] = source[0]
            off_ref[...] = source[1]

    total = [jnp.zeros((8, BLK), F32) for _ in range(SLOTS)]
    for t in range(TB):
        first = by_core((ROW_OF[0][t], ROW_OF[1][t])) * NX + 2 * core
        row = every_ref[first] + every_ref[first + 1]
        rank = sum(
            ((owner_ref[u] == owner_ref[t]).astype(jnp.int32) for u in range(t)), jnp.int32(0)
        )
        for k in range(SLOTS):
            hit = jnp.logical_and(owner_ref[t] == tm, rank == k)
            total[k] = total[k] + jnp.where(hit, row, 0.0)
    for k in range(SLOTS):
        for b in range(8):
            owned_ref[k:k + 1, b * BLK:(b + 1) * BLK] = total[k][b:b + 1, :]


def call(kernel, outs, scratch, flops, *args, scalars=0):
    vmem = pl.BlockSpec(memory_space=pltpu.VMEM)
    smem = pl.BlockSpec(memory_space=pltpu.SMEM)
    moved = sum(a.size * a.dtype.itemsize for a in args)
    return pl.pallas_call(
        kernel,
        out_shape=[jax.ShapeDtypeStruct(s, d) for s, d in outs],
        in_specs=[smem] * scalars + [vmem] * (len(args) - scalars),
        out_specs=[vmem] * len(outs),
        scratch_shapes=[pltpu.VMEM(s, d) for s, d in scratch],
        cost_estimate=pl.CostEstimate(flops=flops, bytes_accessed=moved, transcendentals=0),
        compiler_params=pltpu.CompilerParams(vmem_limit_bytes=24 * 1024 * 1024),
    )(*args)


def sweep(linv, sub, owner):
    flops = 2 * N * N * N
    square, packed, half, tall = ((N, N), BF16), ((512, 1152), BF16), ((512, N), F32), ((N, N), F32)
    part, strip, rows = ((512, N), BF16), ((2, BLK, N), BF16), ((BLK, N), BF16)
    n_tm = lax.axis_size("tm")

    full, short = call(
        pack_kernel, [((BLK, 2 * N), BF16), ((BLK, N + 512), BF16)], [], flops // 64, linv, sub
    )
    q0 = send(full, load_above)
    evens = [send(short, load_from(dx, 0)) for dx in (1, 2, 3)]
    odds = [send(full, load_from(dx, 1)) for dx in (1, 2, 3)]
    gt, ft, fpack, spack = call(
        load_kernel, [square, square, packed, packed], [square, square], 3 * flops,
        full, q0, *evens, *odds,
    )
    to2 = send(spack, replica_to(3, 2))
    gt_next = send(gt, replica_to(1, 0))
    f_next = send(fpack, replica_to(1, 0))
    (second,) = call(step_kernel, [packed], [square, square], 2 * flops, to2, gt, ft)
    to0 = send(second, replica_to(2, 0))
    to1 = send(second, replica_to(2, 1))
    (gram,) = call(gram_kernel, [half], [part], flops, ft)
    (base,) = call(base_kernel, [tall], [square, part, square], 3 * flops, f_next, gt)
    (left,) = call(left_kernel, [square], [part], flops, gt_next, gt)
    own, a1, a2, a3, var = call(
        sweep_kernel, [strip] * 4 + [((n_tm, 8, BLK), F32)],
        [square, square, square, ((8, BLK), F32)],
        6 * flops, to2, to1, to0, left, base, gt_next, gram, gt,
    )
    every = lax.all_to_all(var, "tm", 0, 0, tiled=True)
    b1 = send(a1, spread(False, True))
    b3 = send(a3, spread(True, True))
    b2 = send(a2, spread(True, False))
    return call(
        deliver_kernel, [rows, rows, ((SLOTS, N), F32)], [], flops // 64,
        owner, every, own, b1, b2, b3, scalars=1,
    )


def solution(mesh):
    spec = P(AXES, None)
    return jax.shard_map(
        sweep,
        mesh=mesh,
        in_specs=(spec, spec, P("cfg")),
        out_specs=(spec, spec, spec),
        check_vma=False,
    )
```

```python
import jax
import jax.numpy as jnp
from jax import lax
from jax.experimental import pallas as pl
from jax.experimental.pallas import tpu as pltpu
from jax.sharding import PartitionSpec as P


TB = 4
SLOTS = 2
NX = 4
N = 1024
BLK = 128
AXES = ("cfg", "tm")
ROW_OF = ((0, 3, 5, 6), (0, 2, 4, 7))


NN = (((1,), (0,)), ((), ()))
NT = (((1,), (1,)), ((), ()))
BF16 = jnp.bfloat16
F32 = jnp.float32


def mine(x, core):
    return x // 2 == core


def send(value, fn):
    n_cfg, n_tm = lax.axis_size("cfg"), lax.axis_size("tm")
    route = []
    for cfg in range(n_cfg):
        for tm in range(n_tm):
            y, x = divmod(tm, NX)
            to = fn(x, y, cfg % 2)
            if to is not None:
                route.append((cfg * n_tm + tm, cfg * n_tm + to[1] * NX + to[0]))
    return lax.ppermute(value, AXES, route)


def load_from(dx, parity, groups):
    def fn(x, y, core):
        to = (x - dx) % NX
        if y // 2 in groups and y % 2 == parity and mine(to, core):
            return (to, ROW_OF[core][y // 2])
        return None

    return fn


def load_above(groups):
    def fn(x, y, core):
        if y // 2 in groups and mine(x, core) and y ^ 1 == ROW_OF[core][y // 2]:
            return (x, y ^ 1)
        return None

    return fn


def replica_to(t, u):
    def fn(x, y, core):
        return (x, ROW_OF[core][u]) if mine(x, core) and y == ROW_OF[core][t] else None

    return fn


def spread(across, other):
    def fn(x, y, core):
        if not mine(x, core) or y != ROW_OF[core][y // 2]:
            return None
        return (3 - x if across else x, y ^ 1 if other else y)

    return fn


def block(b):
    return pl.ds(pl.multiple_of(b * BLK, BLK), BLK)


def tile(i):
    return slice(i * 256, (i + 1) * 256)


def here():
    x = lax.rem(lax.axis_index("tm"), NX)
    y = lax.div(lax.axis_index("tm"), NX)
    return x, lax.rem(y, 2), lax.div(y, 2)


def dot(a, b, dims):
    return lax.dot_general(a, b, dims, preferred_element_type=F32)


def pack(pack_ref, s_ref):
    for p in range(4):
        rows = slice(p * BLK, (p + 1) * BLK)
        width = (8 - p) * BLK
        pack_ref[rows, :width] = s_ref[(7 - p) * BLK:(8 - p) * BLK, :width]
        pack_ref[rows, width:] = s_ref[p * BLK:(p + 1) * BLK, :(p + 1) * BLK]


def unpack(s_ref, pack_ref):
    for p in range(4):
        rows = slice(p * BLK, (p + 1) * BLK)
        width = (8 - p) * BLK
        s_ref[(7 - p) * BLK:(8 - p) * BLK, :width] = pack_ref[rows, :width]
        s_ref[p * BLK:(p + 1) * BLK, :(p + 1) * BLK] = pack_ref[rows, width:]


def mirror(s_ref):
    for i in range(1, 8):
        rows = slice(i * BLK, (i + 1) * BLK)
        left = s_ref[rows, :i * BLK].astype(F32)
        s_ref[:i * BLK, rows] = left.T.astype(BF16)


def pack_upper(pack_ref, f_ref):
    for p in range(4):
        rows = slice(p * BLK, (p + 1) * BLK)
        width = (8 - p) * BLK
        pack_ref[rows, :width] = f_ref[p * BLK:(p + 1) * BLK, p * BLK:]
        pack_ref[rows, width:] = f_ref[(7 - p) * BLK:(8 - p) * BLK, (7 - p) * BLK:]


def unpack_upper(f_ref, pack_ref):
    f_ref[...] = jnp.zeros_like(f_ref)
    for p in range(4):
        rows = slice(p * BLK, (p + 1) * BLK)
        width = (8 - p) * BLK
        f_ref[p * BLK:(p + 1) * BLK, p * BLK:] = pack_ref[rows, :width]
        f_ref[(7 - p) * BLK:(8 - p) * BLK, (7 - p) * BLK:] = pack_ref[rows, width:]


def lower(s_ref, f_ref, wt_ref, gt_ref):
    for i in range(4):
        cols = slice(0, (i + 1) * 256)
        gram = dot(f_ref[tile(i), i * 256:], f_ref[cols, i * 256:], NT)
        s_ref[tile(i), cols] = (gram + dot(wt_ref[tile(i), :], gt_ref[cols, :], NT)).astype(BF16)


def pack_kernel(linv_hbm, sub_hbm, full_ref, short_ref, linv_ref, sub_ref, sems):
    copies = [
        pltpu.make_async_copy(linv_hbm, linv_ref, sems.at[0]),
        pltpu.make_async_copy(sub_hbm, sub_ref, sems.at[1]),
    ]
    for copy in copies:
        copy.start()
    for copy in copies:
        copy.wait()
    full_ref[:, :N] = sub_ref[...]
    short_ref[:, :N] = sub_ref[...]
    for b in range(8):
        turned = linv_ref[:, b * BLK:(b + 1) * BLK].astype(F32).T.astype(BF16)
        full_ref[:, N + b * BLK:N + (b + 1) * BLK] = turned
        if b < 4:
            short_ref[:, N + b * BLK:N + (b + 1) * BLK] = turned


def assemble(own, q0, e1, e2, e3, o1, o2, o3, f_ref, l_ref):
    x, parity, _ = here()
    f_ref[512:, :512] = jnp.zeros((512, 512), BF16)

    def place(at, piece, blocks):
        l_ref[block(at), :] = piece[:, :N]
        for b in range(blocks):
            f_ref[b * BLK:(b + 1) * BLK, block(at)] = piece[:, N + b * BLK:N + (b + 1) * BLK]

    place(parity * NX + x, own, 8)
    place((1 - parity) * NX + x, q0, 8)
    for dx, even, odd in ((1, e1, o1), (2, e2, o2), (3, e3, o3)):
        place(lax.rem(x + dx, NX), even, 4)
        place(NX + lax.rem(x + dx, NX), odd, 8)


def couple(gt_ref, f_ref, l_ref):
    for i in range(4):
        gt_ref[tile(i), :] = dot(f_ref[tile(i), i * 256:], l_ref[:, i * 256:], NT).astype(BF16)


def load_kernel(own, q0, e1, e2, e3, o1, o2, o3, gt_ref, f_ref, fpack_ref, spack_ref, l_ref, s_ref):
    assemble(own, q0, e1, e2, e3, o1, o2, o3, f_ref, l_ref)
    couple(gt_ref, f_ref, l_ref)
    lower(s_ref, f_ref, gt_ref, gt_ref)
    pack(spack_ref, s_ref)
    pack_upper(fpack_ref, f_ref)


def late_kernel(own, q0, e1, e2, e3, o1, o2, o3, gt_in, f_in, gt_ref, f_ref, l_ref):
    _, _, group = here()

    @pl.when(group == 0)
    def _():
        assemble(own, q0, e1, e2, e3, o1, o2, o3, f_ref, l_ref)
        couple(gt_ref, f_ref, l_ref)

    @pl.when(group != 0)
    def _():
        gt_ref[...] = gt_in[...]
        f_ref[...] = f_in[...]


def step_kernel(pack_in, gt_ref, f_ref, pack_out, s_ref, wt_ref):
    unpack(s_ref, pack_in)
    mirror(s_ref)
    for i in range(4):
        wt_ref[tile(i), :] = dot(gt_ref[tile(i), :], s_ref[...], NN).astype(BF16)
    lower(s_ref, f_ref, wt_ref, gt_ref)
    pack(pack_out, s_ref)


def rows_of(x, parity):
    far = 3 - x
    return (
        parity * NX + x, (1 - parity) * NX + x, parity * NX + far, (1 - parity) * NX + far
    )


def pick(out_ref, at, ref, places):
    for k, place in enumerate(places):
        out_ref[at + k * BLK:at + (k + 1) * BLK, :] = ref[block(place), :]


def gram_kernel(f_ref, out_ref, fm_ref):
    x, parity, _ = here()
    pick(fm_ref, 0, f_ref, rows_of(x, parity))
    for i in range(2):
        out_ref[tile(i), :] = dot(fm_ref[tile(i), :], f_ref[...], NT)


def base_kernel(fpack_next, gt_ref, base_ref, fn_ref, gm_ref, h_ref):
    x, parity, _ = here()
    places = rows_of(x, parity)
    unpack_upper(fn_ref, fpack_next)
    pick(gm_ref, 0, gt_ref, places)
    pick(h_ref, 512, fn_ref, places)
    for i in range(2):
        h_ref[tile(i), :] = dot(gm_ref[tile(i), :], fn_ref[...], NN).astype(BF16)
    for i in range(4):
        base_ref[tile(i), :] = dot(h_ref[tile(i), :], fn_ref[...], NT)


def left_kernel(gt_next, gt_ref, left_ref, gm_ref):
    x, parity, _ = here()
    places = rows_of(x, parity)
    pick(gm_ref, 0, gt_ref, places)
    pick(left_ref, 512, gt_next, places)
    for i in range(2):
        left_ref[tile(i), :] = dot(gm_ref[tile(i), :], gt_next[...], NN).astype(BF16)


def sweep_kernel(
    to2, to1, to0, left_ref, base_ref, gt_next, gram_ref, gt_ref,
    own_ref, a1_ref, a2_ref, a3_ref, var_ref, s_ref, w_ref, x_ref, d_ref,
):
    x, parity, group = here()
    places = rows_of(x, parity)
    for t, source in ((2, to2), (1, to1), (0, to0)):
        @pl.when(group == t)
        def _():
            unpack(s_ref, source)
            mirror(s_ref)

    @pl.when(group == TB - 1)
    def _():
        for i in range(8):
            row = lax.broadcasted_iota(jnp.int32, (BLK, N), 0) + i * BLK
            col = lax.broadcasted_iota(jnp.int32, (BLK, N), 1)
            s_ref[i * BLK:(i + 1) * BLK, :] = jnp.where(row == col, 1.0, 0.0).astype(BF16)

    @pl.when(group == 0)
    def _():
        for i in range(4):
            w_ref[tile(i), :] = dot(left_ref[tile(i), :], s_ref[...], NN).astype(BF16)
        for i in range(4):
            x_ref[tile(i), :] = (base_ref[tile(i), :] + dot(w_ref[tile(i), :], gt_next[...], NT)).astype(BF16)

    @pl.when(group != 0)
    def _():
        pick(w_ref, 0, gt_ref, places)
        for i in range(2):
            x_ref[tile(i), :] = dot(w_ref[tile(i), :], s_ref[...], NN).astype(BF16)
        pick(x_ref, 512, s_ref, places)

    row = lax.broadcasted_iota(jnp.int32, (BLK, BLK), 0)
    col = lax.broadcasted_iota(jnp.int32, (BLK, BLK), 1)
    d_ref[...] = jnp.zeros_like(d_ref)
    for k, at in enumerate(places):
        rows = slice(k * BLK, (k + 1) * BLK)
        terms = x_ref[rows, :].astype(F32) * gt_ref[block(at), :].astype(F32)
        total = jnp.sum(terms, axis=1, keepdims=True) + gram_ref[rows, block(at)]
        diag = jnp.sum(jnp.where(row == col, total, 0.0), axis=0, keepdims=True)
        d_ref[pl.ds(at, 1), :] = diag.astype(BF16).astype(F32)
    for k in range(var_ref.shape[0]):
        var_ref[k] = d_ref[...]

    outs = (own_ref, a1_ref, a2_ref, a3_ref)
    for i in range(2):
        strip = gram_ref[tile(i), :] + dot(x_ref[tile(i), :], gt_ref[...], NT)
        outs[2 * i][0] = strip[:BLK].astype(BF16)
        outs[2 * i + 1][0] = strip[BLK:].astype(BF16)
        off = -dot(x_ref[tile(i + 2), :], gt_ref[...], NT)
        outs[2 * i][1] = off[:BLK].astype(BF16)
        outs[2 * i + 1][1] = off[BLK:].astype(BF16)


def deliver_kernel(owner_ref, every_ref, own_ref, b1_ref, b2_ref, b3_ref, diag_ref, off_ref, owned_ref):
    x, parity, group = here()
    core = lax.rem(lax.axis_index("cfg"), 2)
    tm = lax.axis_index("tm")

    def by_core(rows):
        return jnp.where(core == 0, rows[0], rows[1])

    level = jnp.int32(0)
    for t in range(TB):
        level = jnp.where(group == t, by_core((ROW_OF[0][t] % 2, ROW_OF[1][t] % 2)), level)
    across = (lax.div(x, 2) != core).astype(jnp.int32)
    way = 2 * across + (parity != level).astype(jnp.int32)
    for k, source in enumerate((own_ref, b1_ref, b2_ref, b3_ref)):
        @pl.when(way == k)
        def _():
            diag_ref[...] = source[0]
            off_ref[...] = source[1]

    total = [jnp.zeros((8, BLK), F32) for _ in range(SLOTS)]
    for t in range(TB):
        first = by_core((ROW_OF[0][t], ROW_OF[1][t])) * NX + 2 * core
        row = every_ref[first] + every_ref[first + 1]
        rank = sum(
            ((owner_ref[u] == owner_ref[t]).astype(jnp.int32) for u in range(t)), jnp.int32(0)
        )
        for k in range(SLOTS):
            hit = jnp.logical_and(owner_ref[t] == tm, rank == k)
            total[k] = total[k] + jnp.where(hit, row, 0.0)
    for k in range(SLOTS):
        for b in range(8):
            owned_ref[k:k + 1, b * BLK:(b + 1) * BLK] = total[k][b:b + 1, :]


def call(kernel, outs, scratch, flops, *args, first=pltpu.VMEM, special=0):
    vmem = pl.BlockSpec(memory_space=pltpu.VMEM)
    moved = sum(a.size * a.dtype.itemsize for a in args)
    return pl.pallas_call(
        kernel,
        out_shape=[jax.ShapeDtypeStruct(s, d) for s, d in outs],
        in_specs=[pl.BlockSpec(memory_space=first)] * special + [vmem] * (len(args) - special),
        out_specs=[vmem] * len(outs),
        scratch_shapes=[pltpu.VMEM(*s) if isinstance(s, tuple) else s for s in scratch],
        cost_estimate=pl.CostEstimate(flops=flops, bytes_accessed=moved, transcendentals=0),
        compiler_params=pltpu.CompilerParams(vmem_limit_bytes=24 * 1024 * 1024),
    )(*args)


def sweep(linv, sub, owner):
    flops = 2 * N * N * N
    square, packed, half, tall = ((N, N), BF16), ((512, 1152), BF16), ((512, N), F32), ((N, N), F32)
    part, strip, rows = ((512, N), BF16), ((2, BLK, N), BF16), ((BLK, N), BF16)
    n_tm = lax.axis_size("tm")

    full, short = call(
        pack_kernel, [((BLK, 2 * N), BF16), ((BLK, N + 512), BF16)],
        [rows, rows, pltpu.SemaphoreType.DMA((2,))], flops // 64, linv, sub,
        first=pltpu.HBM, special=2,
    )

    def load(groups):
        q0 = send(full, load_above(groups))
        odds = [send(full, load_from(dx, 1, groups)) for dx in (1, 2, 3)]
        evens = [send(short, load_from(dx, 0, groups)) for dx in (1, 2, 3)]
        return (full, q0, *evens, *odds)

    pieces = load((1, 2, 3))
    gt_first, ft_first, fpack, spack = call(
        load_kernel, [square, square, packed, packed], [square, square], 3 * flops, *pieces
    )
    to2 = send(spack, replica_to(3, 2))
    gt_next = send(gt_first, replica_to(1, 0))
    f_next = send(fpack, replica_to(1, 0))
    (second,) = call(step_kernel, [packed], [square, square], 2 * flops, to2, gt_first, ft_first)
    pieces = load((0,))
    gt, ft = call(late_kernel, [square, square], [square], flops, *pieces, gt_first, ft_first)
    to0 = send(second, replica_to(2, 0))
    to1 = send(second, replica_to(2, 1))
    (gram,) = call(gram_kernel, [half], [part], flops, ft)
    (base,) = call(base_kernel, [tall], [square, part, square], 3 * flops, f_next, gt)
    (left,) = call(left_kernel, [square], [part], flops, gt_next, gt)
    own, a1, a2, a3, var = call(
        sweep_kernel, [strip] * 4 + [((n_tm, 8, BLK), F32)],
        [square, square, square, ((8, BLK), F32)],
        6 * flops, to2, to1, to0, left, base, gt_next, gram, gt,
    )
    every = lax.all_to_all(var, "tm", 0, 0, tiled=True)
    b1 = send(a1, spread(False, True))
    b3 = send(a3, spread(True, True))
    b2 = send(a2, spread(True, False))
    return call(
        deliver_kernel, [rows, rows, ((SLOTS, N), F32)], [], flops // 64,
        owner, every, own, b1, b2, b3, first=pltpu.SMEM, special=1,
    )


def solution(mesh):
    spec = P(AXES, None)
    return jax.shard_map(
        sweep,
        mesh=mesh,
        in_specs=(spec, spec, P("cfg")),
        out_specs=(spec, spec, spec),
        check_vma=False,
    )
```

```python
import jax
import jax.numpy as jnp
from jax import lax
from jax.experimental import pallas as pl
from jax.experimental.pallas import tpu as pltpu
from jax.sharding import PartitionSpec as P


TB = 4
SLOTS = 2
NX = 4
N = 1024
BLK = 128
AXES = ("cfg", "tm")
ROW_OF = ((0, 3, 5, 6), (0, 2, 4, 7))


NN = (((1,), (0,)), ((), ()))
NT = (((1,), (1,)), ((), ()))
BF16 = jnp.bfloat16
F32 = jnp.float32


def mine(x, core):
    return x // 2 == core


def send(value, fn):
    n_cfg, n_tm = lax.axis_size("cfg"), lax.axis_size("tm")
    route = []
    for cfg in range(n_cfg):
        for tm in range(n_tm):
            y, x = divmod(tm, NX)
            to = fn(x, y, cfg % 2)
            if to is not None:
                route.append((cfg * n_tm + tm, cfg * n_tm + to[1] * NX + to[0]))
    return lax.ppermute(value, AXES, route)


def load_from(dx, parity, groups):
    def fn(x, y, core):
        to = (x - dx) % NX
        if y // 2 in groups and y % 2 == parity and mine(to, core):
            return (to, ROW_OF[core][y // 2])
        return None

    return fn


def late_above(x, y, core):
    return (x, 0) if y == 1 else None


def late_from(dx):
    def fn(x, y, core):
        to = (x - dx) % NX
        return (to, 0) if y == 0 and mine(to, core) else None

    return fn


def load_above(groups):
    def fn(x, y, core):
        if y // 2 in groups and mine(x, core) and y ^ 1 == ROW_OF[core][y // 2]:
            return (x, y ^ 1)
        return None

    return fn


def replica_to(t, u):
    def fn(x, y, core):
        return (x, ROW_OF[core][u]) if mine(x, core) and y == ROW_OF[core][t] else None

    return fn


def spread(across, other):
    def fn(x, y, core):
        if not mine(x, core) or y != ROW_OF[core][y // 2]:
            return None
        return (3 - x if across else x, y ^ 1 if other else y)

    return fn


def block(b):
    return pl.ds(pl.multiple_of(b * BLK, BLK), BLK)


def tile(i):
    return slice(i * 256, (i + 1) * 256)


def here():
    x = lax.rem(lax.axis_index("tm"), NX)
    y = lax.div(lax.axis_index("tm"), NX)
    return x, lax.rem(y, 2), lax.div(y, 2)


def dot(a, b, dims):
    return lax.dot_general(a, b, dims, preferred_element_type=F32)


def pack(pack_ref, s_ref):
    for p in range(4):
        rows = slice(p * BLK, (p + 1) * BLK)
        width = (8 - p) * BLK
        pack_ref[rows, :width] = s_ref[(7 - p) * BLK:(8 - p) * BLK, :width]
        pack_ref[rows, width:] = s_ref[p * BLK:(p + 1) * BLK, :(p + 1) * BLK]


def unpack(s_ref, pack_ref):
    for p in range(4):
        rows = slice(p * BLK, (p + 1) * BLK)
        width = (8 - p) * BLK
        s_ref[(7 - p) * BLK:(8 - p) * BLK, :width] = pack_ref[rows, :width]
        s_ref[p * BLK:(p + 1) * BLK, :(p + 1) * BLK] = pack_ref[rows, width:]


def mirror(s_ref):
    for i in range(1, 8):
        rows = slice(i * BLK, (i + 1) * BLK)
        left = s_ref[rows, :i * BLK].astype(F32)
        s_ref[:i * BLK, rows] = left.T.astype(BF16)


def pack_upper(pack_ref, f_ref):
    for p in range(4):
        rows = slice(p * BLK, (p + 1) * BLK)
        width = (8 - p) * BLK
        pack_ref[rows, :width] = f_ref[p * BLK:(p + 1) * BLK, p * BLK:]
        pack_ref[rows, width:] = f_ref[(7 - p) * BLK:(8 - p) * BLK, (7 - p) * BLK:]


def unpack_upper(f_ref, pack_ref):
    f_ref[...] = jnp.zeros_like(f_ref)
    for p in range(4):
        rows = slice(p * BLK, (p + 1) * BLK)
        width = (8 - p) * BLK
        f_ref[p * BLK:(p + 1) * BLK, p * BLK:] = pack_ref[rows, :width]
        f_ref[(7 - p) * BLK:(8 - p) * BLK, (7 - p) * BLK:] = pack_ref[rows, width:]


def lower(s_ref, f_ref, wt_ref, gt_ref):
    for i in range(4):
        cols = slice(0, (i + 1) * 256)
        gram = dot(f_ref[tile(i), i * 256:], f_ref[cols, i * 256:], NT)
        s_ref[tile(i), cols] = (gram + dot(wt_ref[tile(i), :], gt_ref[cols, :], NT)).astype(BF16)


def pack_kernel(linv_hbm, sub_hbm, full_ref, short_ref, linv_ref, sub_ref, sems):
    copies = [
        pltpu.make_async_copy(linv_hbm, linv_ref, sems.at[0]),
        pltpu.make_async_copy(sub_hbm, sub_ref, sems.at[1]),
    ]
    for copy in copies:
        copy.start()
    for copy in copies:
        copy.wait()
    full_ref[:, :N] = sub_ref[...]
    short_ref[:, :N] = sub_ref[...]
    for b in range(8):
        turned = linv_ref[:, b * BLK:(b + 1) * BLK].astype(F32).T.astype(BF16)
        full_ref[:, N + b * BLK:N + (b + 1) * BLK] = turned
        if b < 4:
            short_ref[:, N + b * BLK:N + (b + 1) * BLK] = turned


def place(at, piece, blocks, f_ref, l_ref):
    l_ref[block(at), :] = piece[:, :N]
    for b in range(blocks):
        f_ref[b * BLK:(b + 1) * BLK, block(at)] = piece[:, N + b * BLK:N + (b + 1) * BLK]


def assemble(own, q0, e1, e2, e3, o1, o2, o3, f_ref, l_ref):
    x, parity, _ = here()
    f_ref[512:, :512] = jnp.zeros((512, 512), BF16)

    place(parity * NX + x, own, 8, f_ref, l_ref)
    place((1 - parity) * NX + x, q0, 8, f_ref, l_ref)
    for dx, even, odd in ((1, e1, o1), (2, e2, o2), (3, e3, o3)):
        place(lax.rem(x + dx, NX), even, 4, f_ref, l_ref)
        place(NX + lax.rem(x + dx, NX), odd, 8, f_ref, l_ref)


def couple(gt_ref, f_ref, l_ref):
    for i in range(4):
        gt_ref[tile(i), :] = dot(f_ref[tile(i), i * 256:], l_ref[:, i * 256:], NT).astype(BF16)


def join_kernel(short_ref, full_ref, out_ref):
    out_ref[:, :N + 512] = short_ref[...]
    out_ref[:, N + 512:] = full_ref[...]


def load_kernel(own, q0, e1, e2, e3, o1, o2, o3, gt_ref, f_ref, fpack_ref, spack_ref, l_ref, s_ref):
    assemble(own, q0, e1, e2, e3, o1, o2, o3, f_ref, l_ref)
    couple(gt_ref, f_ref, l_ref)
    lower(s_ref, f_ref, gt_ref, gt_ref)
    pack(spack_ref, s_ref)
    pack_upper(fpack_ref, f_ref)


def late_kernel(j0, j1, j2, j3, gt_in, f_in, gt_ref, f_ref, l_ref):
    x, _, group = here()

    @pl.when(group == 0)
    def _():
        f_ref[512:, :512] = jnp.zeros((512, 512), BF16)
        for dx, piece in enumerate((j0, j1, j2, j3)):
            at = lax.rem(x + dx, NX)
            place(at, piece[:, :N + 512], 4, f_ref, l_ref)
            place(NX + at, piece[:, N + 512:], 8, f_ref, l_ref)
        couple(gt_ref, f_ref, l_ref)

    @pl.when(group != 0)
    def _():
        gt_ref[...] = gt_in[...]
        f_ref[...] = f_in[...]


def step_kernel(pack_in, gt_ref, f_ref, pack_out, s_ref, wt_ref):
    unpack(s_ref, pack_in)
    mirror(s_ref)
    for i in range(4):
        wt_ref[tile(i), :] = dot(gt_ref[tile(i), :], s_ref[...], NN).astype(BF16)
    lower(s_ref, f_ref, wt_ref, gt_ref)
    pack(pack_out, s_ref)


def rows_of(x, parity):
    far = 3 - x
    return (
        parity * NX + x, (1 - parity) * NX + x, parity * NX + far, (1 - parity) * NX + far
    )


def pick(out_ref, at, ref, places):
    for k, place in enumerate(places):
        out_ref[at + k * BLK:at + (k + 1) * BLK, :] = ref[block(place), :]


def gram_kernel(f_ref, out_ref, fm_ref):
    x, parity, _ = here()
    pick(fm_ref, 0, f_ref, rows_of(x, parity))
    for i in range(2):
        out_ref[tile(i), :] = dot(fm_ref[tile(i), :], f_ref[...], NT)


def base_kernel(fpack_next, gt_ref, base_ref, fn_ref, gm_ref, h_ref):
    x, parity, _ = here()
    places = rows_of(x, parity)
    unpack_upper(fn_ref, fpack_next)
    pick(gm_ref, 0, gt_ref, places)
    pick(h_ref, 512, fn_ref, places)
    for i in range(2):
        h_ref[tile(i), :] = dot(gm_ref[tile(i), :], fn_ref[...], NN).astype(BF16)
    for i in range(4):
        base_ref[tile(i), :] = dot(h_ref[tile(i), :], fn_ref[...], NT)


def left_kernel(gt_next, gt_ref, left_ref, gm_ref):
    x, parity, _ = here()
    places = rows_of(x, parity)
    pick(gm_ref, 0, gt_ref, places)
    pick(left_ref, 512, gt_next, places)
    for i in range(2):
        left_ref[tile(i), :] = dot(gm_ref[tile(i), :], gt_next[...], NN).astype(BF16)


def sweep_kernel(
    to2, to1, to0, left_ref, base_ref, gt_next, gram_ref, gt_ref,
    own_ref, a1_ref, a2_ref, a3_ref, var_ref, s_ref, w_ref, x_ref, d_ref,
):
    x, parity, group = here()
    places = rows_of(x, parity)
    for t, source in ((2, to2), (1, to1), (0, to0)):
        @pl.when(group == t)
        def _():
            unpack(s_ref, source)
            mirror(s_ref)

    @pl.when(group == TB - 1)
    def _():
        for i in range(8):
            row = lax.broadcasted_iota(jnp.int32, (BLK, N), 0) + i * BLK
            col = lax.broadcasted_iota(jnp.int32, (BLK, N), 1)
            s_ref[i * BLK:(i + 1) * BLK, :] = jnp.where(row == col, 1.0, 0.0).astype(BF16)

    @pl.when(group == 0)
    def _():
        for i in range(4):
            w_ref[tile(i), :] = dot(left_ref[tile(i), :], s_ref[...], NN).astype(BF16)
        for i in range(4):
            x_ref[tile(i), :] = (base_ref[tile(i), :] + dot(w_ref[tile(i), :], gt_next[...], NT)).astype(BF16)

    @pl.when(group != 0)
    def _():
        pick(w_ref, 0, gt_ref, places)
        for i in range(2):
            x_ref[tile(i), :] = dot(w_ref[tile(i), :], s_ref[...], NN).astype(BF16)
        pick(x_ref, 512, s_ref, places)

    row = lax.broadcasted_iota(jnp.int32, (BLK, BLK), 0)
    col = lax.broadcasted_iota(jnp.int32, (BLK, BLK), 1)
    d_ref[...] = jnp.zeros_like(d_ref)
    for k, at in enumerate(places):
        rows = slice(k * BLK, (k + 1) * BLK)
        terms = x_ref[rows, :].astype(F32) * gt_ref[block(at), :].astype(F32)
        total = jnp.sum(terms, axis=1, keepdims=True) + gram_ref[rows, block(at)]
        diag = jnp.sum(jnp.where(row == col, total, 0.0), axis=0, keepdims=True)
        d_ref[pl.ds(at, 1), :] = diag.astype(BF16).astype(F32)
    for k in range(var_ref.shape[0]):
        var_ref[k] = d_ref[...]

    outs = (own_ref, a1_ref, a2_ref, a3_ref)
    for i in range(2):
        strip = gram_ref[tile(i), :] + dot(x_ref[tile(i), :], gt_ref[...], NT)
        outs[2 * i][0] = strip[:BLK].astype(BF16)
        outs[2 * i + 1][0] = strip[BLK:].astype(BF16)
        off = -dot(x_ref[tile(i + 2), :], gt_ref[...], NT)
        outs[2 * i][1] = off[:BLK].astype(BF16)
        outs[2 * i + 1][1] = off[BLK:].astype(BF16)


def deliver_kernel(owner_ref, every_ref, own_ref, b1_ref, b2_ref, b3_ref, diag_ref, off_ref, owned_ref):
    x, parity, group = here()
    core = lax.rem(lax.axis_index("cfg"), 2)
    tm = lax.axis_index("tm")

    def by_core(rows):
        return jnp.where(core == 0, rows[0], rows[1])

    level = jnp.int32(0)
    for t in range(TB):
        level = jnp.where(group == t, by_core((ROW_OF[0][t] % 2, ROW_OF[1][t] % 2)), level)
    across = (lax.div(x, 2) != core).astype(jnp.int32)
    way = 2 * across + (parity != level).astype(jnp.int32)
    for k, source in enumerate((own_ref, b1_ref, b2_ref, b3_ref)):
        @pl.when(way == k)
        def _():
            diag_ref[...] = source[0]
            off_ref[...] = source[1]

    total = [jnp.zeros((8, BLK), F32) for _ in range(SLOTS)]
    for t in range(TB):
        first = by_core((ROW_OF[0][t], ROW_OF[1][t])) * NX + 2 * core
        row = every_ref[first] + every_ref[first + 1]
        rank = sum(
            ((owner_ref[u] == owner_ref[t]).astype(jnp.int32) for u in range(t)), jnp.int32(0)
        )
        for k in range(SLOTS):
            hit = jnp.logical_and(owner_ref[t] == tm, rank == k)
            total[k] = total[k] + jnp.where(hit, row, 0.0)
    for k in range(SLOTS):
        for b in range(8):
            owned_ref[k:k + 1, b * BLK:(b + 1) * BLK] = total[k][b:b + 1, :]


def call(kernel, outs, scratch, flops, *args, first=pltpu.VMEM, special=0):
    vmem = pl.BlockSpec(memory_space=pltpu.VMEM)
    moved = sum(a.size * a.dtype.itemsize for a in args)
    return pl.pallas_call(
        kernel,
        out_shape=[jax.ShapeDtypeStruct(s, d) for s, d in outs],
        in_specs=[pl.BlockSpec(memory_space=first)] * special + [vmem] * (len(args) - special),
        out_specs=[vmem] * len(outs),
        scratch_shapes=[pltpu.VMEM(*s) if isinstance(s, tuple) else s for s in scratch],
        cost_estimate=pl.CostEstimate(flops=flops, bytes_accessed=moved, transcendentals=0),
        compiler_params=pltpu.CompilerParams(vmem_limit_bytes=24 * 1024 * 1024),
    )(*args)


def sweep(linv, sub, owner):
    flops = 2 * N * N * N
    square, packed, half, tall = ((N, N), BF16), ((512, 1152), BF16), ((512, N), F32), ((N, N), F32)
    part, strip, rows = ((512, N), BF16), ((2, BLK, N), BF16), ((BLK, N), BF16)
    n_tm = lax.axis_size("tm")

    full, short = call(
        pack_kernel, [((BLK, 2 * N), BF16), ((BLK, N + 512), BF16)],
        [rows, rows, pltpu.SemaphoreType.DMA((2,))], flops // 64, linv, sub,
        first=pltpu.HBM, special=2,
    )

    def load(groups):
        q0 = send(full, load_above(groups))
        odds = [send(full, load_from(dx, 1, groups)) for dx in (1, 2, 3)]
        evens = [send(short, load_from(dx, 0, groups)) for dx in (1, 2, 3)]
        return (full, q0, *evens, *odds)

    pieces = load((1, 2, 3))
    above = send(full, late_above)
    gt_first, ft_first, fpack, spack = call(
        load_kernel, [square, square, packed, packed], [square, square], 3 * flops, *pieces
    )
    to2 = send(spack, replica_to(3, 2))
    gt_next = send(gt_first, replica_to(1, 0))
    f_next = send(fpack, replica_to(1, 0))
    (second,) = call(step_kernel, [packed], [square, square], 2 * flops, to2, gt_first, ft_first)
    (joined,) = call(join_kernel, [((BLK, 3 * N + 512), BF16)], [], flops // 64, short, above)
    pieces = [joined] + [send(joined, late_from(dx)) for dx in (1, 2, 3)]
    gt, ft = call(late_kernel, [square, square], [square], flops, *pieces, gt_first, ft_first)
    to0 = send(second, replica_to(2, 0))
    to1 = send(second, replica_to(2, 1))
    (gram,) = call(gram_kernel, [half], [part], flops, ft)
    (base,) = call(base_kernel, [tall], [square, part, square], 3 * flops, f_next, gt)
    (left,) = call(left_kernel, [square], [part], flops, gt_next, gt)
    own, a1, a2, a3, var = call(
        sweep_kernel, [strip] * 4 + [((n_tm, 8, BLK), F32)],
        [square, square, square, ((8, BLK), F32)],
        6 * flops, to2, to1, to0, left, base, gt_next, gram, gt,
    )
    every = lax.all_to_all(var, "tm", 0, 0, tiled=True)
    b1 = send(a1, spread(False, True))
    b3 = send(a3, spread(True, True))
    b2 = send(a2, spread(True, False))
    return call(
        deliver_kernel, [rows, rows, ((SLOTS, N), F32)], [], flops // 64,
        owner, every, own, b1, b2, b3, first=pltpu.SMEM, special=1,
    )


def solution(mesh):
    spec = P(AXES, None)
    return jax.shard_map(
        sweep,
        mesh=mesh,
        in_specs=(spec, spec, P("cfg")),
        out_specs=(spec, spec, spec),
        check_vma=False,
    )
```

```python
import jax
import jax.numpy as jnp
from jax import lax
from jax.experimental import pallas as pl
from jax.experimental.pallas import tpu as pltpu
from jax.sharding import PartitionSpec as P


TB = 4
SLOTS = 2
NX = 4
N = 1024
BLK = 128
AXES = ("cfg", "tm")
ROW_OF = ((0, 3, 5, 6), (0, 2, 4, 7))


NN = (((1,), (0,)), ((), ()))
NT = (((1,), (1,)), ((), ()))
BF16 = jnp.bfloat16
F32 = jnp.float32


def mine(x, core):
    return x // 2 == core


def send(value, fn):
    n_cfg, n_tm = lax.axis_size("cfg"), lax.axis_size("tm")
    route = []
    for cfg in range(n_cfg):
        for tm in range(n_tm):
            y, x = divmod(tm, NX)
            to = fn(x, y, cfg % 2)
            if to is not None:
                route.append((cfg * n_tm + tm, cfg * n_tm + to[1] * NX + to[0]))
    return lax.ppermute(value, AXES, route)


def load_from(dx, parity, groups):
    def fn(x, y, core):
        to = (x - dx) % NX
        if y // 2 in groups and y % 2 == parity and mine(to, core):
            return (to, ROW_OF[core][y // 2])
        return None

    return fn


def late_above(x, y, core):
    return (x, 0) if y == 1 else None


def late_from(dx):
    def fn(x, y, core):
        to = (x - dx) % NX
        return (to, 0) if y == 0 and mine(to, core) else None

    return fn


def load_above(groups):
    def fn(x, y, core):
        if y // 2 in groups and mine(x, core) and y ^ 1 == ROW_OF[core][y // 2]:
            return (x, y ^ 1)
        return None

    return fn


def replica_to(t, u):
    def fn(x, y, core):
        return (x, ROW_OF[core][u]) if mine(x, core) and y == ROW_OF[core][t] else None

    return fn


def spread(across, other):
    def fn(x, y, core):
        if not mine(x, core) or y != ROW_OF[core][y // 2]:
            return None
        return (3 - x if across else x, y ^ 1 if other else y)

    return fn


def block(b):
    return pl.ds(pl.multiple_of(b * BLK, BLK), BLK)


def tile(i):
    return slice(i * 256, (i + 1) * 256)


def here():
    x = lax.rem(lax.axis_index("tm"), NX)
    y = lax.div(lax.axis_index("tm"), NX)
    return x, lax.rem(y, 2), lax.div(y, 2)


def dot(a, b, dims):
    return lax.dot_general(a, b, dims, preferred_element_type=F32)


def pack(pack_ref, s_ref):
    for p in range(4):
        rows = slice(p * BLK, (p + 1) * BLK)
        width = (8 - p) * BLK
        pack_ref[rows, :width] = s_ref[(7 - p) * BLK:(8 - p) * BLK, :width]
        pack_ref[rows, width:] = s_ref[p * BLK:(p + 1) * BLK, :(p + 1) * BLK]


def unpack(s_ref, pack_ref):
    for p in range(4):
        rows = slice(p * BLK, (p + 1) * BLK)
        width = (8 - p) * BLK
        s_ref[(7 - p) * BLK:(8 - p) * BLK, :width] = pack_ref[rows, :width]
        s_ref[p * BLK:(p + 1) * BLK, :(p + 1) * BLK] = pack_ref[rows, width:]


def mirror(s_ref):
    for i in range(1, 8):
        rows = slice(i * BLK, (i + 1) * BLK)
        left = s_ref[rows, :i * BLK].astype(F32)
        s_ref[:i * BLK, rows] = left.T.astype(BF16)


def pack_upper(pack_ref, f_ref):
    for p in range(4):
        rows = slice(p * BLK, (p + 1) * BLK)
        width = (8 - p) * BLK
        pack_ref[rows, :width] = f_ref[p * BLK:(p + 1) * BLK, p * BLK:]
        pack_ref[rows, width:] = f_ref[(7 - p) * BLK:(8 - p) * BLK, (7 - p) * BLK:]


def unpack_upper(f_ref, pack_ref):
    f_ref[...] = jnp.zeros_like(f_ref)
    for p in range(4):
        rows = slice(p * BLK, (p + 1) * BLK)
        width = (8 - p) * BLK
        f_ref[p * BLK:(p + 1) * BLK, p * BLK:] = pack_ref[rows, :width]
        f_ref[(7 - p) * BLK:(8 - p) * BLK, (7 - p) * BLK:] = pack_ref[rows, width:]


def gram_tile(f_ref, i):
    return dot(f_ref[tile(i), i * 256:], f_ref[:(i + 1) * 256, i * 256:], NT)


def sweep_tile(wt_ref, gt_ref, i):
    return dot(wt_ref[tile(i), :], gt_ref[:(i + 1) * 256, :], NT)


def pack_kernel(linv_hbm, sub_hbm, full_ref, short_ref, linv_ref, sub_ref, sems):
    copies = [
        pltpu.make_async_copy(linv_hbm, linv_ref, sems.at[0]),
        pltpu.make_async_copy(sub_hbm, sub_ref, sems.at[1]),
    ]
    for copy in copies:
        copy.start()
    for copy in copies:
        copy.wait()
    full_ref[:, :N] = sub_ref[...]
    short_ref[:, :N] = sub_ref[...]
    for b in range(8):
        turned = linv_ref[:, b * BLK:(b + 1) * BLK].astype(F32).T.astype(BF16)
        full_ref[:, N + b * BLK:N + (b + 1) * BLK] = turned
        if b < 4:
            short_ref[:, N + b * BLK:N + (b + 1) * BLK] = turned


def place(at, piece, blocks, f_ref, l_ref):
    l_ref[block(at), :] = piece[:, :N]
    for b in range(blocks):
        f_ref[b * BLK:(b + 1) * BLK, block(at)] = piece[:, N + b * BLK:N + (b + 1) * BLK]


def assemble(own, q0, e1, e2, e3, o1, o2, o3, f_ref, l_ref):
    x, parity, _ = here()
    f_ref[512:, :512] = jnp.zeros((512, 512), BF16)

    place(parity * NX + x, own, 8, f_ref, l_ref)
    place((1 - parity) * NX + x, q0, 8, f_ref, l_ref)
    for dx, even, odd in ((1, e1, o1), (2, e2, o2), (3, e3, o3)):
        place(lax.rem(x + dx, NX), even, 4, f_ref, l_ref)
        place(NX + lax.rem(x + dx, NX), odd, 8, f_ref, l_ref)


def couple(gt_ref, f_ref, l_ref):
    for i in range(4):
        gt_ref[tile(i), :] = dot(f_ref[tile(i), i * 256:], l_ref[:, i * 256:], NT).astype(BF16)


def join_kernel(short_ref, full_ref, out_ref):
    out_ref[:, :N + 512] = short_ref[...]
    out_ref[:, N + 512:] = full_ref[...]


def load_kernel(own, q0, e1, e2, e3, o1, o2, o3, gt_ref, f_ref, fpack_ref, spack_ref, l_ref, s_ref):
    _, _, group = here()
    assemble(own, q0, e1, e2, e3, o1, o2, o3, f_ref, l_ref)
    couple(gt_ref, f_ref, l_ref)

    @pl.when(group == TB - 1)
    def _():
        for i in range(4):
            s_ref[tile(i), :(i + 1) * 256] = (
                gram_tile(f_ref, i) + sweep_tile(gt_ref, gt_ref, i)
            ).astype(BF16)
        pack(spack_ref, s_ref)

    @pl.when(group != TB - 1)
    def _():
        pack_upper(fpack_ref, f_ref)


def late_kernel(j0, j1, j2, j3, gt_in, f_in, gt_ref, f_ref, l_ref):
    x, _, group = here()

    @pl.when(group == 0)
    def _():
        f_ref[512:, :512] = jnp.zeros((512, 512), BF16)
        for dx, piece in enumerate((j0, j1, j2, j3)):
            at = lax.rem(x + dx, NX)
            place(at, piece[:, :N + 512], 4, f_ref, l_ref)
            place(NX + at, piece[:, N + 512:], 8, f_ref, l_ref)
        couple(gt_ref, f_ref, l_ref)

    @pl.when(group != 0)
    def _():
        gt_ref[...] = gt_in[...]
        f_ref[...] = f_in[...]


def lower_kernel(f_ref, low_ref):
    for i in range(4):
        low_ref[tile(i), :(i + 1) * 256] = gram_tile(f_ref, i)


def step_kernel(pack_in, gt_ref, low_ref, pack_out, s_ref, wt_ref):
    unpack(s_ref, pack_in)
    mirror(s_ref)
    for i in range(4):
        wt_ref[tile(i), :] = dot(gt_ref[tile(i), :], s_ref[...], NN).astype(BF16)
    for i in range(4):
        s_ref[tile(i), :(i + 1) * 256] = (
            low_ref[tile(i), :(i + 1) * 256] + sweep_tile(wt_ref, gt_ref, i)
        ).astype(BF16)
    pack(pack_out, s_ref)


def rows_of(x, parity):
    far = 3 - x
    return (
        parity * NX + x, (1 - parity) * NX + x, parity * NX + far, (1 - parity) * NX + far
    )


def pick(out_ref, at, ref, places):
    for k, place in enumerate(places):
        out_ref[at + k * BLK:at + (k + 1) * BLK, :] = ref[block(place), :]


def gram_kernel(f_ref, out_ref, fm_ref):
    x, parity, _ = here()
    pick(fm_ref, 0, f_ref, rows_of(x, parity))
    for i in range(2):
        out_ref[tile(i), :] = dot(fm_ref[tile(i), :], f_ref[...], NT)


def base_kernel(fpack_next, gt_ref, base_ref, fn_ref, gm_ref, h_ref):
    x, parity, _ = here()
    places = rows_of(x, parity)
    unpack_upper(fn_ref, fpack_next)
    pick(gm_ref, 0, gt_ref, places)
    pick(h_ref, 512, fn_ref, places)
    for i in range(2):
        h_ref[tile(i), :] = dot(gm_ref[tile(i), :], fn_ref[...], NN).astype(BF16)
    for i in range(4):
        base_ref[tile(i), :] = dot(h_ref[tile(i), :], fn_ref[...], NT)


def left_kernel(gt_next, gt_ref, left_ref, gm_ref):
    x, parity, _ = here()
    places = rows_of(x, parity)
    pick(gm_ref, 0, gt_ref, places)
    pick(left_ref, 512, gt_next, places)
    for i in range(2):
        left_ref[tile(i), :] = dot(gm_ref[tile(i), :], gt_next[...], NN).astype(BF16)


def sweep_kernel(
    to2, to1, to0, left_ref, base_ref, gt_next, gram_ref, gt_ref,
    own_ref, a1_ref, a2_ref, a3_ref, var_ref, s_ref, w_ref, x_ref, d_ref,
):
    x, parity, group = here()
    places = rows_of(x, parity)
    for t, source in ((2, to2), (1, to1), (0, to0)):
        @pl.when(group == t)
        def _():
            unpack(s_ref, source)
            mirror(s_ref)

    @pl.when(group == TB - 1)
    def _():
        for i in range(8):
            row = lax.broadcasted_iota(jnp.int32, (BLK, N), 0) + i * BLK
            col = lax.broadcasted_iota(jnp.int32, (BLK, N), 1)
            s_ref[i * BLK:(i + 1) * BLK, :] = jnp.where(row == col, 1.0, 0.0).astype(BF16)

    @pl.when(group == 0)
    def _():
        for i in range(4):
            w_ref[tile(i), :] = dot(left_ref[tile(i), :], s_ref[...], NN).astype(BF16)
        for i in range(4):
            x_ref[tile(i), :] = (base_ref[tile(i), :] + dot(w_ref[tile(i), :], gt_next[...], NT)).astype(BF16)

    @pl.when(group != 0)
    def _():
        pick(w_ref, 0, gt_ref, places)
        for i in range(2):
            x_ref[tile(i), :] = dot(w_ref[tile(i), :], s_ref[...], NN).astype(BF16)
        pick(x_ref, 512, s_ref, places)

    row = lax.broadcasted_iota(jnp.int32, (BLK, BLK), 0)
    col = lax.broadcasted_iota(jnp.int32, (BLK, BLK), 1)
    d_ref[...] = jnp.zeros_like(d_ref)
    for k, at in enumerate(places):
        rows = slice(k * BLK, (k + 1) * BLK)
        terms = x_ref[rows, :].astype(F32) * gt_ref[block(at), :].astype(F32)
        total = jnp.sum(terms, axis=1, keepdims=True) + gram_ref[rows, block(at)]
        diag = jnp.sum(jnp.where(row == col, total, 0.0), axis=0, keepdims=True)
        d_ref[pl.ds(at, 1), :] = diag.astype(BF16).astype(F32)
    for k in range(var_ref.shape[0]):
        var_ref[k] = d_ref[...]

    outs = (own_ref, a1_ref, a2_ref, a3_ref)
    for i in range(2):
        strip = gram_ref[tile(i), :] + dot(x_ref[tile(i), :], gt_ref[...], NT)
        outs[2 * i][0] = strip[:BLK].astype(BF16)
        outs[2 * i + 1][0] = strip[BLK:].astype(BF16)
        off = -dot(x_ref[tile(i + 2), :], gt_ref[...], NT)
        outs[2 * i][1] = off[:BLK].astype(BF16)
        outs[2 * i + 1][1] = off[BLK:].astype(BF16)


def deliver_kernel(owner_ref, every_ref, own_ref, b1_ref, b2_ref, b3_ref, diag_ref, off_ref, owned_ref):
    x, parity, group = here()
    core = lax.rem(lax.axis_index("cfg"), 2)
    tm = lax.axis_index("tm")

    def by_core(rows):
        return jnp.where(core == 0, rows[0], rows[1])

    level = jnp.int32(0)
    for t in range(TB):
        level = jnp.where(group == t, by_core((ROW_OF[0][t] % 2, ROW_OF[1][t] % 2)), level)
    across = (lax.div(x, 2) != core).astype(jnp.int32)
    way = 2 * across + (parity != level).astype(jnp.int32)
    for k, source in enumerate((own_ref, b1_ref, b2_ref, b3_ref)):
        @pl.when(way == k)
        def _():
            diag_ref[...] = source[0]
            off_ref[...] = source[1]

    total = [jnp.zeros((8, BLK), F32) for _ in range(SLOTS)]
    for t in range(TB):
        first = by_core((ROW_OF[0][t], ROW_OF[1][t])) * NX + 2 * core
        row = every_ref[first] + every_ref[first + 1]
        rank = sum(
            ((owner_ref[u] == owner_ref[t]).astype(jnp.int32) for u in range(t)), jnp.int32(0)
        )
        for k in range(SLOTS):
            hit = jnp.logical_and(owner_ref[t] == tm, rank == k)
            total[k] = total[k] + jnp.where(hit, row, 0.0)
    for k in range(SLOTS):
        for b in range(8):
            owned_ref[k:k + 1, b * BLK:(b + 1) * BLK] = total[k][b:b + 1, :]


def call(kernel, outs, scratch, flops, *args, first=pltpu.VMEM, special=0, grant=24 << 20):
    vmem = pl.BlockSpec(memory_space=pltpu.VMEM)
    moved = sum(a.size * a.dtype.itemsize for a in args)
    return pl.pallas_call(
        kernel,
        out_shape=[jax.ShapeDtypeStruct(s, d) for s, d in outs],
        in_specs=[pl.BlockSpec(memory_space=first)] * special + [vmem] * (len(args) - special),
        out_specs=[vmem] * len(outs),
        scratch_shapes=[pltpu.VMEM(*s) if isinstance(s, tuple) else s for s in scratch],
        cost_estimate=pl.CostEstimate(flops=flops, bytes_accessed=moved, transcendentals=0),
        compiler_params=pltpu.CompilerParams(vmem_limit_bytes=grant),
    )(*args)


def sweep(linv, sub, owner):
    flops = 2 * N * N * N
    square, packed, half, tall = ((N, N), BF16), ((512, 1152), BF16), ((512, N), F32), ((N, N), F32)
    part, strip, rows = ((512, N), BF16), ((2, BLK, N), BF16), ((BLK, N), BF16)
    n_tm = lax.axis_size("tm")

    full, short = call(
        pack_kernel, [((BLK, 2 * N), BF16), ((BLK, N + 512), BF16)],
        [rows, rows, pltpu.SemaphoreType.DMA((2,))], flops // 64, linv, sub,
        first=pltpu.HBM, special=2, grant=24 << 20,
    )

    def load(groups):
        q0 = send(full, load_above(groups))
        odds = [send(full, load_from(dx, 1, groups)) for dx in (1, 2, 3)]
        evens = [send(short, load_from(dx, 0, groups)) for dx in (1, 2, 3)]
        return (full, q0, *evens, *odds)

    pieces = load((1, 2, 3))
    above = send(full, late_above)
    gt_first, ft_first, fpack, spack = call(
        load_kernel, [square, square, packed, packed], [square, square], 3 * flops, *pieces
    )
    to2 = send(spack, replica_to(3, 2))
    gt_next = send(gt_first, replica_to(1, 0))
    f_next = send(fpack, replica_to(1, 0))
    (low,) = call(lower_kernel, [tall], [], flops // 2, ft_first)
    (second,) = call(step_kernel, [packed], [square, square], 2 * flops, to2, gt_first, low)
    (joined,) = call(join_kernel, [((BLK, 3 * N + 512), BF16)], [], flops // 64, short, above)
    pieces = [joined] + [send(joined, late_from(dx)) for dx in (1, 2, 3)]
    gt, ft = call(late_kernel, [square, square], [square], flops, *pieces, gt_first, ft_first)
    to0 = send(second, replica_to(2, 0))
    to1 = send(second, replica_to(2, 1))
    (gram,) = call(gram_kernel, [half], [part], flops, ft)
    (base,) = call(base_kernel, [tall], [square, part, square], 3 * flops, f_next, gt)
    (left,) = call(left_kernel, [square], [part], flops, gt_next, gt)
    own, a1, a2, a3, var = call(
        sweep_kernel, [strip] * 4 + [((n_tm, 8, BLK), F32)],
        [square, square, square, ((8, BLK), F32)],
        6 * flops, to2, to1, to0, left, base, gt_next, gram, gt,
    )
    every = lax.all_to_all(var, "tm", 0, 0, tiled=True)
    b1 = send(a1, spread(False, True))
    b3 = send(a3, spread(True, True))
    b2 = send(a2, spread(True, False))
    return call(
        deliver_kernel, [rows, rows, ((SLOTS, N), F32)], [], flops // 64,
        owner, every, own, b1, b2, b3, first=pltpu.SMEM, special=1,
    )


def solution(mesh):
    spec = P(AXES, None)
    return jax.shard_map(
        sweep,
        mesh=mesh,
        in_specs=(spec, spec, P("cfg")),
        out_specs=(spec, spec, spec),
        check_vma=False,
    )
```

```python
import jax
import jax.numpy as jnp
from jax import lax
from jax.experimental import pallas as pl
from jax.experimental.pallas import tpu as pltpu
from jax.sharding import PartitionSpec as P


TB = 4
SLOTS = 2
NX = 4
N = 1024
BLK = 128
AXES = ("cfg", "tm")
ROW_OF = ((0, 3, 5, 6), (0, 2, 4, 7))


NN = (((1,), (0,)), ((), ()))
NT = (((1,), (1,)), ((), ()))
BF16 = jnp.bfloat16
F32 = jnp.float32


def mine(x, core):
    return x // 2 == core


def send(value, fn):
    n_cfg, n_tm = lax.axis_size("cfg"), lax.axis_size("tm")
    route = []
    for cfg in range(n_cfg):
        for tm in range(n_tm):
            y, x = divmod(tm, NX)
            to = fn(x, y, cfg % 2)
            if to is not None:
                route.append((cfg * n_tm + tm, cfg * n_tm + to[1] * NX + to[0]))
    return lax.ppermute(value, AXES, route)


def load_from(dx, parity, groups):
    def fn(x, y, core):
        to = (x - dx) % NX
        if y // 2 in groups and y % 2 == parity and mine(to, core):
            return (to, ROW_OF[core][y // 2])
        return None

    return fn


def late_above(x, y, core):
    return (x, 0) if y == 1 else None


def late_from(dx):
    def fn(x, y, core):
        to = (x - dx) % NX
        return (to, 0) if y == 0 and mine(to, core) else None

    return fn


def load_above(groups):
    def fn(x, y, core):
        if y // 2 in groups and mine(x, core) and y ^ 1 == ROW_OF[core][y // 2]:
            return (x, y ^ 1)
        return None

    return fn


def replica_to(t, u):
    def fn(x, y, core):
        return (x, ROW_OF[core][u]) if mine(x, core) and y == ROW_OF[core][t] else None

    return fn


def spread(across, other):
    def fn(x, y, core):
        if not mine(x, core) or y != ROW_OF[core][y // 2]:
            return None
        return (3 - x if across else x, y ^ 1 if other else y)

    return fn


def block(b):
    return pl.ds(pl.multiple_of(b * BLK, BLK), BLK)


def tile(i):
    return slice(i * 256, (i + 1) * 256)


def here():
    x = lax.rem(lax.axis_index("tm"), NX)
    y = lax.div(lax.axis_index("tm"), NX)
    return x, lax.rem(y, 2), lax.div(y, 2)


def dot(a, b, dims):
    return lax.dot_general(a, b, dims, preferred_element_type=F32)


def pack(pack_ref, s_ref):
    for p in range(4):
        rows = slice(p * BLK, (p + 1) * BLK)
        width = (8 - p) * BLK
        pack_ref[rows, :width] = s_ref[(7 - p) * BLK:(8 - p) * BLK, :width]
        pack_ref[rows, width:] = s_ref[p * BLK:(p + 1) * BLK, :(p + 1) * BLK]


def unpack(s_ref, pack_ref):
    for p in range(4):
        rows = slice(p * BLK, (p + 1) * BLK)
        width = (8 - p) * BLK
        s_ref[(7 - p) * BLK:(8 - p) * BLK, :width] = pack_ref[rows, :width]
        s_ref[p * BLK:(p + 1) * BLK, :(p + 1) * BLK] = pack_ref[rows, width:]


def mirror(s_ref):
    for i in range(1, 8):
        rows = slice(i * BLK, (i + 1) * BLK)
        left = s_ref[rows, :i * BLK].astype(F32)
        s_ref[:i * BLK, rows] = left.T.astype(BF16)


def pack_upper(pack_ref, f_ref):
    for p in range(4):
        rows = slice(p * BLK, (p + 1) * BLK)
        width = (8 - p) * BLK
        pack_ref[rows, :width] = f_ref[p * BLK:(p + 1) * BLK, p * BLK:]
        pack_ref[rows, width:] = f_ref[(7 - p) * BLK:(8 - p) * BLK, (7 - p) * BLK:]


def unpack_upper(f_ref, pack_ref):
    f_ref[...] = jnp.zeros_like(f_ref)
    for p in range(4):
        rows = slice(p * BLK, (p + 1) * BLK)
        width = (8 - p) * BLK
        f_ref[p * BLK:(p + 1) * BLK, p * BLK:] = pack_ref[rows, :width]
        f_ref[(7 - p) * BLK:(8 - p) * BLK, (7 - p) * BLK:] = pack_ref[rows, width:]


def gram_tile(f_ref, i):
    return dot(f_ref[tile(i), i * 256:], f_ref[:(i + 1) * 256, i * 256:], NT)


def sweep_tile(wt_ref, gt_ref, i):
    return dot(wt_ref[tile(i), :], gt_ref[:(i + 1) * 256, :], NT)


def pack_kernel(linv_hbm, sub_hbm, full_ref, short_ref, linv_ref, sub_ref, sems):
    copies = [
        pltpu.make_async_copy(linv_hbm, linv_ref, sems.at[0]),
        pltpu.make_async_copy(sub_hbm, sub_ref, sems.at[1]),
    ]
    for copy in copies:
        copy.start()
    for copy in copies:
        copy.wait()
    full_ref[:, :N] = sub_ref[...]
    short_ref[:, :N] = sub_ref[...]
    for b in range(8):
        turned = linv_ref[:, b * BLK:(b + 1) * BLK].astype(F32).T.astype(BF16)
        full_ref[:, N + b * BLK:N + (b + 1) * BLK] = turned
        if b < 4:
            short_ref[:, N + b * BLK:N + (b + 1) * BLK] = turned


def place(at, piece, blocks, f_ref, l_ref):
    l_ref[block(at), :] = piece[:, :N]
    for b in range(blocks):
        f_ref[b * BLK:(b + 1) * BLK, block(at)] = piece[:, N + b * BLK:N + (b + 1) * BLK]


def assemble(own, q0, e1, e2, e3, o1, o2, o3, f_ref, l_ref):
    x, parity, _ = here()
    f_ref[512:, :512] = jnp.zeros((512, 512), BF16)

    place(parity * NX + x, own, 8, f_ref, l_ref)
    place((1 - parity) * NX + x, q0, 8, f_ref, l_ref)
    for dx, even, odd in ((1, e1, o1), (2, e2, o2), (3, e3, o3)):
        place(lax.rem(x + dx, NX), even, 4, f_ref, l_ref)
        place(NX + lax.rem(x + dx, NX), odd, 8, f_ref, l_ref)


def couple(gt_ref, f_ref, l_ref):
    for i in range(4):
        gt_ref[tile(i), :] = dot(f_ref[tile(i), i * 256:], l_ref[:, i * 256:], NT).astype(BF16)


def join_kernel(short_ref, full_ref, out_ref):
    out_ref[:, :N + 512] = short_ref[...]
    out_ref[:, N + 512:] = full_ref[...]


def load_kernel(own, q0, e1, e2, e3, o1, o2, o3, gt_ref, f_ref, fpack_ref, spack_ref, l_ref, s_ref):
    _, _, group = here()
    assemble(own, q0, e1, e2, e3, o1, o2, o3, f_ref, l_ref)
    couple(gt_ref, f_ref, l_ref)

    @pl.when(group == TB - 1)
    def _():
        for i in range(4):
            s_ref[tile(i), :(i + 1) * 256] = (
                gram_tile(f_ref, i) + sweep_tile(gt_ref, gt_ref, i)
            ).astype(BF16)
        pack(spack_ref, s_ref)

    @pl.when(group != TB - 1)
    def _():
        pack_upper(fpack_ref, f_ref)


def late_kernel(j0, j1, j2, j3, gt_in, f_in, gt_ref, f_ref, l_ref):
    x, _, group = here()

    @pl.when(group == 0)
    def _():
        f_ref[512:, :512] = jnp.zeros((512, 512), BF16)
        for dx, piece in enumerate((j0, j1, j2, j3)):
            at = lax.rem(x + dx, NX)
            place(at, piece[:, :N + 512], 4, f_ref, l_ref)
            place(NX + at, piece[:, N + 512:], 8, f_ref, l_ref)
        couple(gt_ref, f_ref, l_ref)

    @pl.when(group != 0)
    def _():
        gt_ref[...] = gt_in[...]
        f_ref[...] = f_in[...]


def lower_kernel(f_ref, low_ref):
    for i in range(4):
        low_ref[tile(i), :(i + 1) * 256] = gram_tile(f_ref, i)


def step_kernel(pack_in, gt_ref, low_ref, pack_out, s_ref, wt_ref):
    unpack(s_ref, pack_in)
    mirror(s_ref)
    for i in range(4):
        wt_ref[tile(i), :] = dot(gt_ref[tile(i), :], s_ref[...], NN).astype(BF16)
    for i in range(4):
        s_ref[tile(i), :(i + 1) * 256] = (
            low_ref[tile(i), :(i + 1) * 256] + sweep_tile(wt_ref, gt_ref, i)
        ).astype(BF16)
    pack(pack_out, s_ref)


def rows_of(x, parity):
    far = 3 - x
    return (
        parity * NX + x, (1 - parity) * NX + x, parity * NX + far, (1 - parity) * NX + far
    )


def pick(out_ref, at, ref, places):
    for k, place in enumerate(places):
        out_ref[at + k * BLK:at + (k + 1) * BLK, :] = ref[block(place), :]


def gram_kernel(f_ref, out_ref, fm_ref):
    x, parity, _ = here()
    pick(fm_ref, 0, f_ref, rows_of(x, parity))
    for i in range(2):
        out_ref[tile(i), :] = dot(fm_ref[tile(i), :], f_ref[...], NT)


def base_kernel(fpack_next, gt_ref, base_ref, fn_ref, gm_ref, h_ref):
    x, parity, _ = here()
    places = rows_of(x, parity)
    unpack_upper(fn_ref, fpack_next)
    pick(gm_ref, 0, gt_ref, places)
    pick(h_ref, 512, fn_ref, places)
    for i in range(2):
        h_ref[tile(i), :] = dot(gm_ref[tile(i), :], fn_ref[...], NN).astype(BF16)
    for i in range(4):
        base_ref[tile(i), :] = dot(h_ref[tile(i), :], fn_ref[...], NT)


def left_kernel(gt_next, gt_ref, left_ref, gm_ref):
    x, parity, _ = here()
    places = rows_of(x, parity)
    pick(gm_ref, 0, gt_ref, places)
    pick(left_ref, 512, gt_next, places)
    for i in range(2):
        left_ref[tile(i), :] = dot(gm_ref[tile(i), :], gt_next[...], NN).astype(BF16)


def sweep_kernel(
    to2, to1, to0, left_ref, base_ref, gt_next, gram_ref, gt_ref,
    own_ref, a1_ref, a2_ref, a3_ref, var_ref, s_ref, w_ref, x_ref, d_ref,
):
    x, parity, group = here()
    places = rows_of(x, parity)
    for t, source in ((2, to2), (1, to1), (0, to0)):
        @pl.when(group == t)
        def _():
            unpack(s_ref, source)
            mirror(s_ref)

    @pl.when(group == TB - 1)
    def _():
        for i in range(8):
            row = lax.broadcasted_iota(jnp.int32, (BLK, N), 0) + i * BLK
            col = lax.broadcasted_iota(jnp.int32, (BLK, N), 1)
            s_ref[i * BLK:(i + 1) * BLK, :] = jnp.where(row == col, 1.0, 0.0).astype(BF16)

    @pl.when(group == 0)
    def _():
        for i in range(4):
            w_ref[tile(i), :] = dot(left_ref[tile(i), :], s_ref[...], NN).astype(BF16)
        for i in range(4):
            x_ref[tile(i), :] = (base_ref[tile(i), :] + dot(w_ref[tile(i), :], gt_next[...], NT)).astype(BF16)

    @pl.when(group != 0)
    def _():
        pick(w_ref, 0, gt_ref, places)
        for i in range(2):
            x_ref[tile(i), :] = dot(w_ref[tile(i), :], s_ref[...], NN).astype(BF16)
        pick(x_ref, 512, s_ref, places)

    row = lax.broadcasted_iota(jnp.int32, (BLK, BLK), 0)
    col = lax.broadcasted_iota(jnp.int32, (BLK, BLK), 1)
    d_ref[...] = jnp.zeros_like(d_ref)
    for k, at in enumerate(places):
        rows = slice(k * BLK, (k + 1) * BLK)
        terms = x_ref[rows, :].astype(F32) * gt_ref[block(at), :].astype(F32)
        total = jnp.sum(terms, axis=1, keepdims=True) + gram_ref[rows, block(at)]
        diag = jnp.sum(jnp.where(row == col, total, 0.0), axis=0, keepdims=True)
        d_ref[pl.ds(at, 1), :] = diag.astype(BF16).astype(F32)
    for k in range(var_ref.shape[0]):
        var_ref[k] = d_ref[...]

    outs = (own_ref, a1_ref, a2_ref, a3_ref)
    for i in range(2):
        strip = gram_ref[tile(i), :] + dot(x_ref[tile(i), :], gt_ref[...], NT)
        outs[2 * i][0] = strip[:BLK].astype(BF16)
        outs[2 * i + 1][0] = strip[BLK:].astype(BF16)
        off = -dot(x_ref[tile(i + 2), :], gt_ref[...], NT)
        outs[2 * i][1] = off[:BLK].astype(BF16)
        outs[2 * i + 1][1] = off[BLK:].astype(BF16)


def deliver_kernel(owner_ref, every_ref, own_ref, b1_ref, b2_ref, b3_ref, diag_ref, off_ref, owned_ref):
    x, parity, group = here()
    core = lax.rem(lax.axis_index("cfg"), 2)
    tm = lax.axis_index("tm")

    def by_core(rows):
        return jnp.where(core == 0, rows[0], rows[1])

    level = jnp.int32(0)
    for t in range(TB):
        level = jnp.where(group == t, by_core((ROW_OF[0][t] % 2, ROW_OF[1][t] % 2)), level)
    across = (lax.div(x, 2) != core).astype(jnp.int32)
    way = 2 * across + (parity != level).astype(jnp.int32)
    for k, source in enumerate((own_ref, b1_ref, b2_ref, b3_ref)):
        @pl.when(way == k)
        def _():
            diag_ref[...] = source[0]
            off_ref[...] = source[1]

    total = [jnp.zeros((8, BLK), F32) for _ in range(SLOTS)]
    for t in range(TB):
        first = by_core((ROW_OF[0][t], ROW_OF[1][t])) * NX + 2 * core
        row = every_ref[first] + every_ref[first + 1]
        rank = sum(
            ((owner_ref[u] == owner_ref[t]).astype(jnp.int32) for u in range(t)), jnp.int32(0)
        )
        for k in range(SLOTS):
            hit = jnp.logical_and(owner_ref[t] == tm, rank == k)
            total[k] = total[k] + jnp.where(hit, row, 0.0)
    for k in range(SLOTS):
        for b in range(8):
            owned_ref[k:k + 1, b * BLK:(b + 1) * BLK] = total[k][b:b + 1, :]


def call(kernel, outs, scratch, flops, *args, first=pltpu.VMEM, special=0, grant=24 << 20):
    vmem = pl.BlockSpec(memory_space=pltpu.VMEM)
    moved = sum(a.size * a.dtype.itemsize for a in args)
    return pl.pallas_call(
        kernel,
        out_shape=[jax.ShapeDtypeStruct(s, d) for s, d in outs],
        in_specs=[pl.BlockSpec(memory_space=first)] * special + [vmem] * (len(args) - special),
        out_specs=[vmem] * len(outs),
        scratch_shapes=[pltpu.VMEM(*s) if isinstance(s, tuple) else s for s in scratch],
        cost_estimate=pl.CostEstimate(flops=flops, bytes_accessed=moved, transcendentals=0),
        compiler_params=pltpu.CompilerParams(vmem_limit_bytes=grant),
    )(*args)


def sweep(linv, sub, owner):
    flops = 2 * N * N * N
    square, packed, half, tall = ((N, N), BF16), ((512, 1152), BF16), ((512, N), F32), ((N, N), F32)
    part, strip, rows = ((512, N), BF16), ((2, BLK, N), BF16), ((BLK, N), BF16)
    n_tm = lax.axis_size("tm")

    full, short = call(
        pack_kernel, [((BLK, 2 * N), BF16), ((BLK, N + 512), BF16)],
        [rows, rows, pltpu.SemaphoreType.DMA((2,))], flops // 64, linv, sub,
        first=pltpu.HBM, special=2, grant=24 << 20,
    )

    def load(groups):
        q0 = send(full, load_above(groups))
        odds, evens = [], []
        for dx in (1, 2, 3):
            odds.append(send(full, load_from(dx, 1, groups)))
            evens.append(send(short, load_from(dx, 0, groups)))
        return (full, q0, *evens, *odds)

    pieces = load((1, 2, 3))
    above = send(full, late_above)
    gt_first, ft_first, fpack, spack = call(
        load_kernel, [square, square, packed, packed], [square, square], 3 * flops, *pieces
    )
    to2 = send(spack, replica_to(3, 2))
    gt_next = send(gt_first, replica_to(1, 0))
    f_next = send(fpack, replica_to(1, 0))
    (low,) = call(lower_kernel, [tall], [], flops // 2, ft_first)
    (second,) = call(step_kernel, [packed], [square, square], 2 * flops, to2, gt_first, low)
    (joined,) = call(join_kernel, [((BLK, 3 * N + 512), BF16)], [], flops // 64, short, above)
    pieces = [joined] + [send(joined, late_from(dx)) for dx in (1, 2, 3)]
    gt, ft = call(late_kernel, [square, square], [square], flops, *pieces, gt_first, ft_first)
    to0 = send(second, replica_to(2, 0))
    to1 = send(second, replica_to(2, 1))
    (gram,) = call(gram_kernel, [half], [part], flops, ft)
    (base,) = call(base_kernel, [tall], [square, part, square], 3 * flops, f_next, gt)
    (left,) = call(left_kernel, [square], [part], flops, gt_next, gt)
    own, a1, a2, a3, var = call(
        sweep_kernel, [strip] * 4 + [((n_tm, 8, BLK), F32)],
        [square, square, square, ((8, BLK), F32)],
        6 * flops, to2, to1, to0, left, base, gt_next, gram, gt,
    )
    every = lax.all_to_all(var, "tm", 0, 0, tiled=True)
    b1 = send(a1, spread(False, True))
    b3 = send(a3, spread(True, True))
    b2 = send(a2, spread(True, False))
    return call(
        deliver_kernel, [rows, rows, ((SLOTS, N), F32)], [], flops // 64,
        owner, every, own, b1, b2, b3, first=pltpu.SMEM, special=1,
    )


def solution(mesh):
    spec = P(AXES, None)
    return jax.shard_map(
        sweep,
        mesh=mesh,
        in_specs=(spec, spec, P("cfg")),
        out_specs=(spec, spec, spec),
        check_vma=False,
    )
```

```python
import jax
import jax.numpy as jnp
from jax import lax
from jax.experimental import pallas as pl
from jax.experimental.pallas import tpu as pltpu
from jax.sharding import PartitionSpec as P


TB = 4
SLOTS = 2
NX = 4
N = 1024
BLK = 128
AXES = ("cfg", "tm")
ROW_OF = ((0, 3, 5, 6), (0, 2, 4, 7))


NN = (((1,), (0,)), ((), ()))
NT = (((1,), (1,)), ((), ()))
BF16 = jnp.bfloat16
F32 = jnp.float32


def mine(x, core):
    return x // 2 == core


def send(value, fn):
    n_cfg, n_tm = lax.axis_size("cfg"), lax.axis_size("tm")
    route = []
    for cfg in range(n_cfg):
        for tm in range(n_tm):
            y, x = divmod(tm, NX)
            to = fn(x, y, cfg % 2)
            if to is not None:
                route.append((cfg * n_tm + tm, cfg * n_tm + to[1] * NX + to[0]))
    return lax.ppermute(value, AXES, route)


def load_from(dx, parity, groups):
    def fn(x, y, core):
        to = (x - dx) % NX
        if y // 2 in groups and y % 2 == parity and mine(to, core):
            return (to, ROW_OF[core][y // 2])
        return None

    return fn


def late_above(x, y, core):
    return (x, 0) if y == 1 else None


def late_from(dx):
    def fn(x, y, core):
        to = (x - dx) % NX
        return (to, 0) if y == 0 and mine(to, core) else None

    return fn


def load_above(groups):
    def fn(x, y, core):
        if y // 2 in groups and mine(x, core) and y ^ 1 == ROW_OF[core][y // 2]:
            return (x, y ^ 1)
        return None

    return fn


def replica_to(t, u):
    def fn(x, y, core):
        return (x, ROW_OF[core][u]) if mine(x, core) and y == ROW_OF[core][t] else None

    return fn


def spread(across, other):
    def fn(x, y, core):
        if not mine(x, core) or y != ROW_OF[core][y // 2]:
            return None
        return (3 - x if across else x, y ^ 1 if other else y)

    return fn


def block(b):
    return pl.ds(pl.multiple_of(b * BLK, BLK), BLK)


def tile(i):
    return slice(i * 256, (i + 1) * 256)


def here():
    x = lax.rem(lax.axis_index("tm"), NX)
    y = lax.div(lax.axis_index("tm"), NX)
    return x, lax.rem(y, 2), lax.div(y, 2)


def dot(a, b, dims):
    return lax.dot_general(a, b, dims, preferred_element_type=F32)


def pack(pack_ref, s_ref):
    for p in range(4):
        rows = slice(p * BLK, (p + 1) * BLK)
        width = (8 - p) * BLK
        pack_ref[rows, :width] = s_ref[(7 - p) * BLK:(8 - p) * BLK, :width]
        pack_ref[rows, width:] = s_ref[p * BLK:(p + 1) * BLK, :(p + 1) * BLK]


def unpack(s_ref, pack_ref):
    for p in range(4):
        rows = slice(p * BLK, (p + 1) * BLK)
        width = (8 - p) * BLK
        s_ref[(7 - p) * BLK:(8 - p) * BLK, :width] = pack_ref[rows, :width]
        s_ref[p * BLK:(p + 1) * BLK, :(p + 1) * BLK] = pack_ref[rows, width:]


def mirror(s_ref):
    for i in range(1, 8):
        rows = slice(i * BLK, (i + 1) * BLK)
        left = s_ref[rows, :i * BLK].astype(F32)
        s_ref[:i * BLK, rows] = left.T.astype(BF16)


def pack_upper(pack_ref, f_ref):
    for p in range(4):
        rows = slice(p * BLK, (p + 1) * BLK)
        width = (8 - p) * BLK
        pack_ref[rows, :width] = f_ref[p * BLK:(p + 1) * BLK, p * BLK:]
        pack_ref[rows, width:] = f_ref[(7 - p) * BLK:(8 - p) * BLK, (7 - p) * BLK:]


def unpack_upper(f_ref, pack_ref):
    f_ref[...] = jnp.zeros_like(f_ref)
    for p in range(4):
        rows = slice(p * BLK, (p + 1) * BLK)
        width = (8 - p) * BLK
        f_ref[p * BLK:(p + 1) * BLK, p * BLK:] = pack_ref[rows, :width]
        f_ref[(7 - p) * BLK:(8 - p) * BLK, (7 - p) * BLK:] = pack_ref[rows, width:]


def gram_tile(f_ref, i):
    return dot(f_ref[tile(i), i * 256:], f_ref[:(i + 1) * 256, i * 256:], NT)


def sweep_tile(wt_ref, gt_ref, i):
    return dot(wt_ref[tile(i), :], gt_ref[:(i + 1) * 256, :], NT)


def pack_kernel(linv_hbm, sub_hbm, full_ref, short_ref, linv_ref, sub_ref, sems):
    copies = [
        pltpu.make_async_copy(linv_hbm, linv_ref, sems.at[0]),
        pltpu.make_async_copy(sub_hbm, sub_ref, sems.at[1]),
    ]
    for copy in copies:
        copy.start()
    for copy in copies:
        copy.wait()
    full_ref[:, :N] = sub_ref[...]
    short_ref[:, :N] = sub_ref[...]
    for b in range(8):
        turned = linv_ref[:, b * BLK:(b + 1) * BLK].astype(F32).T.astype(BF16)
        full_ref[:, N + b * BLK:N + (b + 1) * BLK] = turned
        if b < 4:
            short_ref[:, N + b * BLK:N + (b + 1) * BLK] = turned


def place(at, piece, blocks, f_ref, l_ref):
    l_ref[block(at), :] = piece[:, :N]
    for b in range(blocks):
        f_ref[b * BLK:(b + 1) * BLK, block(at)] = piece[:, N + b * BLK:N + (b + 1) * BLK]


def assemble(own, q0, e1, e2, e3, o1, o2, o3, f_ref, l_ref):
    x, parity, _ = here()
    f_ref[512:, :512] = jnp.zeros((512, 512), BF16)

    place(parity * NX + x, own, 8, f_ref, l_ref)
    place((1 - parity) * NX + x, q0, 8, f_ref, l_ref)
    for dx, even, odd in ((1, e1, o1), (2, e2, o2), (3, e3, o3)):
        place(lax.rem(x + dx, NX), even, 4, f_ref, l_ref)
        place(NX + lax.rem(x + dx, NX), odd, 8, f_ref, l_ref)


def couple(gt_ref, f_ref, l_ref):
    for i in range(4):
        gt_ref[tile(i), :] = dot(f_ref[tile(i), i * 256:], l_ref[:, i * 256:], NT).astype(BF16)


def join_kernel(short_ref, full_ref, out_ref):
    out_ref[:, :N + 512] = short_ref[...]
    out_ref[:, N + 512:] = full_ref[...]


def load_kernel(own, q0, e1, e2, e3, o1, o2, o3, gt_ref, f_ref, fpack_ref, spack_ref, l_ref, s_ref):
    _, _, group = here()
    assemble(own, q0, e1, e2, e3, o1, o2, o3, f_ref, l_ref)
    couple(gt_ref, f_ref, l_ref)

    @pl.when(group == TB - 1)
    def _():
        for i in range(4):
            s_ref[tile(i), :(i + 1) * 256] = (
                gram_tile(f_ref, i) + sweep_tile(gt_ref, gt_ref, i)
            ).astype(BF16)
        pack(spack_ref, s_ref)

    @pl.when(group != TB - 1)
    def _():
        pack_upper(fpack_ref, f_ref)


def late_kernel(j0, j1, j2, j3, gt_in, f_in, gt_ref, f_ref, l_ref):
    x, _, group = here()

    @pl.when(group == 0)
    def _():
        f_ref[512:, :512] = jnp.zeros((512, 512), BF16)
        for dx, piece in enumerate((j0, j1, j2, j3)):
            at = lax.rem(x + dx, NX)
            place(at, piece[:, :N + 512], 4, f_ref, l_ref)
            place(NX + at, piece[:, N + 512:], 8, f_ref, l_ref)
        couple(gt_ref, f_ref, l_ref)

    @pl.when(group != 0)
    def _():
        gt_ref[...] = gt_in[...]
        f_ref[...] = f_in[...]


def lower_kernel(f_ref, low_ref):
    for i in range(4):
        low_ref[tile(i), :(i + 1) * 256] = gram_tile(f_ref, i)


def step_kernel(pack_in, gt_ref, low_ref, pack_out, s_ref, wt_ref):
    unpack(s_ref, pack_in)
    mirror(s_ref)
    for i in range(4):
        wt_ref[tile(i), :] = dot(gt_ref[tile(i), :], s_ref[...], NN).astype(BF16)
    for i in range(4):
        s_ref[tile(i), :(i + 1) * 256] = (
            low_ref[tile(i), :(i + 1) * 256] + sweep_tile(wt_ref, gt_ref, i)
        ).astype(BF16)
    pack(pack_out, s_ref)


def rows_of(x, parity):
    far = 3 - x
    return (
        parity * NX + x, (1 - parity) * NX + x, parity * NX + far, (1 - parity) * NX + far
    )


def pick(out_ref, at, ref, places):
    for k, place in enumerate(places):
        out_ref[at + k * BLK:at + (k + 1) * BLK, :] = ref[block(place), :]


def gram_kernel(f_ref, out_ref, fm_ref):
    x, parity, _ = here()
    pick(fm_ref, 0, f_ref, rows_of(x, parity))
    for i in range(2):
        out_ref[tile(i), :] = dot(fm_ref[tile(i), :], f_ref[...], NT)


def base_kernel(fpack_next, gt_ref, base_ref, fn_ref, gm_ref, h_ref):
    x, parity, _ = here()
    places = rows_of(x, parity)
    unpack_upper(fn_ref, fpack_next)
    pick(gm_ref, 0, gt_ref, places)
    pick(h_ref, 512, fn_ref, places)
    for i in range(2):
        h_ref[tile(i), :] = dot(gm_ref[tile(i), :], fn_ref[...], NN).astype(BF16)
    for i in range(4):
        base_ref[tile(i), :] = dot(h_ref[tile(i), :], fn_ref[...], NT)


def left_kernel(gt_next, gt_ref, left_ref, gm_ref):
    x, parity, _ = here()
    places = rows_of(x, parity)
    pick(gm_ref, 0, gt_ref, places)
    pick(left_ref, 512, gt_next, places)
    for i in range(2):
        left_ref[tile(i), :] = dot(gm_ref[tile(i), :], gt_next[...], NN).astype(BF16)


def sweep_kernel(
    to2, to1, to0, left_ref, base_ref, gt_next, gram_ref, gt_ref,
    own_ref, a1_ref, a2_ref, a3_ref, var_ref, s_ref, w_ref, x_ref, d_ref,
):
    x, parity, group = here()
    places = rows_of(x, parity)
    for t, source in ((2, to2), (1, to1), (0, to0)):
        @pl.when(group == t)
        def _():
            unpack(s_ref, source)
            mirror(s_ref)

    @pl.when(group == TB - 1)
    def _():
        for i in range(8):
            row = lax.broadcasted_iota(jnp.int32, (BLK, N), 0) + i * BLK
            col = lax.broadcasted_iota(jnp.int32, (BLK, N), 1)
            s_ref[i * BLK:(i + 1) * BLK, :] = jnp.where(row == col, 1.0, 0.0).astype(BF16)

    @pl.when(group == 0)
    def _():
        for i in range(4):
            w_ref[tile(i), :] = dot(left_ref[tile(i), :], s_ref[...], NN).astype(BF16)
        for i in range(4):
            x_ref[tile(i), :] = (base_ref[tile(i), :] + dot(w_ref[tile(i), :], gt_next[...], NT)).astype(BF16)

    @pl.when(group != 0)
    def _():
        pick(w_ref, 0, gt_ref, places)
        for i in range(2):
            x_ref[tile(i), :] = dot(w_ref[tile(i), :], s_ref[...], NN).astype(BF16)
        pick(x_ref, 512, s_ref, places)

    row = lax.broadcasted_iota(jnp.int32, (BLK, BLK), 0)
    col = lax.broadcasted_iota(jnp.int32, (BLK, BLK), 1)
    d_ref[...] = jnp.zeros_like(d_ref)
    for k, at in enumerate(places):
        rows = slice(k * BLK, (k + 1) * BLK)
        terms = x_ref[rows, :].astype(F32) * gt_ref[block(at), :].astype(F32)
        total = jnp.sum(terms, axis=1, keepdims=True) + gram_ref[rows, block(at)]
        diag = jnp.sum(jnp.where(row == col, total, 0.0), axis=0, keepdims=True)
        d_ref[pl.ds(at, 1), :] = diag.astype(BF16).astype(F32)
    for k in range(var_ref.shape[0]):
        var_ref[k] = d_ref[...].astype(BF16)

    outs = (own_ref, a1_ref, a2_ref, a3_ref)
    for i in range(2):
        strip = gram_ref[tile(i), :] + dot(x_ref[tile(i), :], gt_ref[...], NT)
        outs[2 * i][0] = strip[:BLK].astype(BF16)
        outs[2 * i + 1][0] = strip[BLK:].astype(BF16)
        off = -dot(x_ref[tile(i + 2), :], gt_ref[...], NT)
        outs[2 * i][1] = off[:BLK].astype(BF16)
        outs[2 * i + 1][1] = off[BLK:].astype(BF16)


def deliver_kernel(owner_ref, every_ref, own_ref, b1_ref, b2_ref, b3_ref, diag_ref, off_ref, owned_ref):
    x, parity, group = here()
    core = lax.rem(lax.axis_index("cfg"), 2)
    tm = lax.axis_index("tm")

    def by_core(rows):
        return jnp.where(core == 0, rows[0], rows[1])

    level = jnp.int32(0)
    for t in range(TB):
        level = jnp.where(group == t, by_core((ROW_OF[0][t] % 2, ROW_OF[1][t] % 2)), level)
    across = (lax.div(x, 2) != core).astype(jnp.int32)
    way = 2 * across + (parity != level).astype(jnp.int32)
    for k, source in enumerate((own_ref, b1_ref, b2_ref, b3_ref)):
        @pl.when(way == k)
        def _():
            diag_ref[...] = source[0]
            off_ref[...] = source[1]

    total = [jnp.zeros((8, BLK), F32) for _ in range(SLOTS)]
    for t in range(TB):
        first = by_core((ROW_OF[0][t], ROW_OF[1][t])) * NX + 2 * core
        row = every_ref[first].astype(F32) + every_ref[first + 1].astype(F32)
        rank = sum(
            ((owner_ref[u] == owner_ref[t]).astype(jnp.int32) for u in range(t)), jnp.int32(0)
        )
        for k in range(SLOTS):
            hit = jnp.logical_and(owner_ref[t] == tm, rank == k)
            total[k] = total[k] + jnp.where(hit, row, 0.0)
    for k in range(SLOTS):
        for b in range(8):
            owned_ref[k:k + 1, b * BLK:(b + 1) * BLK] = total[k][b:b + 1, :]


def call(kernel, outs, scratch, flops, *args, first=pltpu.VMEM, special=0, grant=24 << 20):
    vmem = pl.BlockSpec(memory_space=pltpu.VMEM)
    moved = sum(a.size * a.dtype.itemsize for a in args)
    return pl.pallas_call(
        kernel,
        out_shape=[jax.ShapeDtypeStruct(s, d) for s, d in outs],
        in_specs=[pl.BlockSpec(memory_space=first)] * special + [vmem] * (len(args) - special),
        out_specs=[vmem] * len(outs),
        scratch_shapes=[pltpu.VMEM(*s) if isinstance(s, tuple) else s for s in scratch],
        cost_estimate=pl.CostEstimate(flops=flops, bytes_accessed=moved, transcendentals=0),
        compiler_params=pltpu.CompilerParams(vmem_limit_bytes=grant),
    )(*args)


def sweep(linv, sub, owner):
    flops = 2 * N * N * N
    square, packed, half, tall = ((N, N), BF16), ((512, 1152), BF16), ((512, N), F32), ((N, N), F32)
    part, strip, rows = ((512, N), BF16), ((2, BLK, N), BF16), ((BLK, N), BF16)
    n_tm = lax.axis_size("tm")

    full, short = call(
        pack_kernel, [((BLK, 2 * N), BF16), ((BLK, N + 512), BF16)],
        [rows, rows, pltpu.SemaphoreType.DMA((2,))], flops // 64, linv, sub,
        first=pltpu.HBM, special=2, grant=24 << 20,
    )

    def load(groups):
        q0 = send(full, load_above(groups))
        odds, evens = [], []
        for dx in (1, 2, 3):
            odds.append(send(full, load_from(dx, 1, groups)))
            evens.append(send(short, load_from(dx, 0, groups)))
        return (full, q0, *evens, *odds)

    pieces = load((1, 2, 3))
    above = send(full, late_above)
    gt_first, ft_first, fpack, spack = call(
        load_kernel, [square, square, packed, packed], [square, square], 3 * flops, *pieces
    )
    to2 = send(spack, replica_to(3, 2))
    gt_next = send(gt_first, replica_to(1, 0))
    f_next = send(fpack, replica_to(1, 0))
    (low,) = call(lower_kernel, [tall], [], flops // 2, ft_first)
    (second,) = call(step_kernel, [packed], [square, square], 2 * flops, to2, gt_first, low)
    (joined,) = call(join_kernel, [((BLK, 3 * N + 512), BF16)], [], flops // 64, short, above)
    pieces = [joined] + [send(joined, late_from(dx)) for dx in (1, 2, 3)]
    gt, ft = call(late_kernel, [square, square], [square], flops, *pieces, gt_first, ft_first)
    to0 = send(second, replica_to(2, 0))
    to1 = send(second, replica_to(2, 1))
    (gram,) = call(gram_kernel, [half], [part], flops, ft)
    (base,) = call(base_kernel, [tall], [square, part, square], 3 * flops, f_next, gt)
    (left,) = call(left_kernel, [square], [part], flops, gt_next, gt)
    own, a1, a2, a3, var = call(
        sweep_kernel, [strip] * 4 + [((n_tm, 8, BLK), BF16)],
        [square, square, square, ((8, BLK), F32)],
        6 * flops, to2, to1, to0, left, base, gt_next, gram, gt,
    )
    every = lax.all_to_all(var, "tm", 0, 0, tiled=True)
    b1 = send(a1, spread(False, True))
    b3 = send(a3, spread(True, True))
    b2 = send(a2, spread(True, False))
    return call(
        deliver_kernel, [rows, rows, ((SLOTS, N), F32)], [], flops // 64,
        owner, every, own, b1, b2, b3, first=pltpu.SMEM, special=1,
    )


def solution(mesh):
    spec = P(AXES, None)
    return jax.shard_map(
        sweep,
        mesh=mesh,
        in_specs=(spec, spec, P("cfg")),
        out_specs=(spec, spec, spec),
        check_vma=False,
    )
```
